32 devices in a mesh: rep: 8 (over y, x, core), shard: 4 (over z).
Axes of the slice: x: 2, y: 2, z: 4, core: 2. Of those that a mesh axis runs over, the one named last changes fastest.
Arguments:
- activations: bfloat16 [6, 4096, 2048], P(None, ('rep', 'shard')), may hold values from -50 to 50
- cotangents: bfloat16 [6, 4096, 512], P(None, ('rep', 'shard')), may hold values from -120 to 120
- momentum: float32 [12, 256, 2048], P(None, None, 'shard'), may hold values from -6 to 6
- owners: int32 [12], replicated, may hold values from 0 to 3, as said below
- bucket_starts: int32 [2], replicated, may hold values from 1 to 11, as said below
Outputs:
- momentum_out: float32 [12, 256, 2048], P(None, None, 'shard')
- update: float32 [12, 256, 2048], P(None, None, 'shard')
- owned: bfloat16 [16, 256, 2048], P('shard')
The draws below stay inside these ranges and needn't reach their ends.
Inputs may be any that keep to these rules, and one draw needn't show every extreme that they name: `owners`: no owner is named more than 4 times, and some owner exactly 4 times. `bucket_starts`: strictly increasing.
All inputs are finite; a program needn't handle non-finite values.
Results may differ from the reference program's by a relative error of at most 0.033.
Values may be sent and summed in bfloat16 or wider, within the bound.
A program may use at most 128 MiB of HBM per device.

```python
import math
import jax
import jax.numpy as jnp
from jax import lax

D = 2048
KV = 256
LAYERS = 6
ITERS = 5
BUCKETS = 3
MATS = 12
SLOTS = 4
TOKENS = 4096
N_SHARD = 4


def bucket_layout(key):
    key_starts = jax.random.fold_in(key, 31)
    chosen = jax.random.permutation(key_starts, MATS - 2)[:BUCKETS - 2] + 1
    last_start = jnp.full((1,), MATS - 1, dtype=jnp.int32)
    return jnp.sort(jnp.concatenate([chosen.astype(jnp.int32), last_start])).astype(jnp.int32)


def draw_activations(key, part):
    key_values = jax.random.fold_in(key, 41)
    shape_full = (LAYERS, TOKENS, D)
    values = jnp.clip(jax.random.normal(key_values, shape_full, jnp.float32), -4.5, 4.5)
    ratio = 6.0
    position = jnp.arange(D, dtype=jnp.float32) / D
    rising = jnp.exp(math.log(ratio) * position)
    mean_energy = (ratio * ratio - 1.0) / (2.0 * math.log(ratio))
    column_scale = rising / math.sqrt(mean_energy)
    return (values * column_scale[None, None, :]).astype(jnp.bfloat16)


def draw_cotangents(key, part):
    key_normal = jax.random.fold_in(key, 11)
    key_quiet_scale = jax.random.fold_in(key, 12)
    key_column = jax.random.fold_in(key, 13)
    key_quiet = jax.random.fold_in(key, 14)
    key_loud_scale = jax.random.fold_in(key, 15)
    shape_full = (LAYERS, TOKENS, 2 * KV)
    normal_part = jnp.clip(jax.random.normal(key_normal, shape_full, jnp.float32), -5.0, 5.0)
    starts = bucket_layout(key)
    indices = jnp.arange(MATS, dtype=jnp.int32)
    buckets = jnp.sum((indices[:, None] >= starts[None, :]).astype(jnp.int32), axis=1)
    quiet_bucket = jax.random.randint(key_quiet, (), 0, BUCKETS, dtype=jnp.int32)
    quiet_log = jax.random.uniform(key_quiet_scale, (MATS,), jnp.float32, math.log(0.03), math.log(0.1))
    loud_log = jax.random.uniform(key_loud_scale, (MATS,), jnp.float32, 0.0, math.log(8.0))
    matrix_scale = jnp.exp(jnp.where(buckets == quiet_bucket, quiet_log, loud_log))
    matrix_scale = jnp.repeat(matrix_scale.reshape(LAYERS, 1, 2), KV, axis=2)
    column_scale = jnp.exp(jax.random.uniform(key_column, (LAYERS, 1, 2 * KV), jnp.float32, 0.0, math.log(3.0)))
    return (normal_part * matrix_scale * column_scale).astype(jnp.bfloat16)


def draw_owners(key, part):
    key_first = jax.random.fold_in(key, 21)
    key_second = jax.random.fold_in(key, 22)
    key_third = jax.random.fold_in(key, 23)
    shuffled = jax.random.permutation(key_first, N_SHARD).astype(jnp.int32)
    filled = jnp.full((SLOTS,), shuffled[0], dtype=jnp.int32)
    others = jax.random.permutation(key_second, jnp.repeat(shuffled[1:], SLOTS))
    candidates = jnp.concatenate([filled, others])[:MATS]
    return jax.random.permutation(key_third, candidates).astype(jnp.int32)


def draw_bucket_starts(key, part):
    return bucket_layout(key)


def block_scale(rng, shape, pieces, smallest, largest):
    level = 1.0
    for axis_at, shards_of in pieces:
        steps = jax.random.uniform(jax.random.fold_in(jax.random.fold_in(rng, 6), axis_at), (shards_of,), jnp.float32, smallest / len(pieces), largest / len(pieces))
        level = level * jnp.repeat(jnp.exp(steps), shape[axis_at] // shards_of).reshape((-1,) + (1,) * (len(shape) - 1 - axis_at))
    return level


def bell_draw(stream_key, extent, deviation, limit, shards=(), kind=jnp.bfloat16):
    drawn = jax.random.normal(stream_key, extent, jnp.float32) * deviation
    if len(shards) > 0:
        drawn = block_scale(stream_key, extent, shards, -0.22, 0.18) * drawn
    return jnp.clip(drawn, min=-limit, max=limit).astype(kind)


def setup_inputs(seed: int = 0) -> dict:
    key_list = jax.random.split(jax.random.key(seed), 6)
    activations = draw_activations(jax.random.fold_in(key_list[5], 71), 0)
    cotangents = draw_cotangents(jax.random.fold_in(key_list[5], 71), 0)
    momentum = bell_draw(key_list[2], (MATS, KV, D), 1.0, 6.0, ((2, 4),), jnp.float32)
    owners = draw_owners(jax.random.fold_in(key_list[5], 71), 0)
    bucket_starts = draw_bucket_starts(jax.random.fold_in(key_list[5], 71), 0)
    return {"activations": activations, "cotangents": cotangents, "momentum": momentum, "owners": owners, "bucket_starts": bucket_starts}


coef_a = 3.4445
coef_b = -4.775
coef_c = 2.0315
momentum_rate = 0.95
clip_level = 0.5
epsilon = 1e-06

def orthogonal(update_in):
    values = update_in.astype(jnp.float32)
    frobenius = jnp.sqrt(jnp.sum(values * values))
    matrix = (values / (frobenius + epsilon)).astype(jnp.bfloat16)
    for iteration in range(ITERS):
        gram_matrix = jnp.dot(matrix, matrix.T, preferred_element_type=jnp.float32).astype(jnp.bfloat16)
        square = jnp.dot(gram_matrix, gram_matrix, preferred_element_type=jnp.float32)
        mixing = (coef_b * gram_matrix.astype(jnp.float32) + coef_c * square).astype(jnp.bfloat16)
        matrix = (coef_a * matrix.astype(jnp.float32) + jnp.dot(mixing, matrix, preferred_element_type=jnp.float32)).astype(jnp.bfloat16)
    return matrix

def clip_factors(square_sums, bucket_starts):
    indices = jnp.arange(MATS, dtype=jnp.int32)
    buckets = lax.optimization_barrier(jnp.sum((indices[:, None] >= bucket_starts[None, :]).astype(jnp.int32), axis=1))
    together = (buckets[:, None] == buckets[None, :]).astype(jnp.float32)
    totals = lax.optimization_barrier(jnp.sum(together * square_sums[None, :], axis=1))
    members = lax.optimization_barrier(jnp.sum(together, axis=1))
    root_mean = jnp.sqrt(totals / (members * KV * D) + epsilon)
    return jnp.minimum(1.0, clip_level / root_mean)

def slot_numbers(owners):
    indices = jnp.arange(MATS, dtype=jnp.int32)
    earlier = (indices[None, :] < indices[:, None]) & (owners[None, :] == owners[:, None])
    return lax.optimization_barrier(jnp.sum(earlier.astype(jnp.int32), axis=1)).astype(jnp.int32)

def reference(activations, cotangents, momentum, owners, bucket_starts):
    layer_grads = []
    for layer_index in range(LAYERS):
        layer_grads.append(lax.dot_general(cotangents[layer_index], activations[layer_index], (((0,), (0,)), ((), ())), preferred_element_type=jnp.float32))
    gradient = jnp.stack(layer_grads).reshape(MATS, KV, D) / jnp.sqrt(jnp.float32(TOKENS))
    square_sums = lax.optimization_barrier(jnp.sum(gradient * gradient, axis=(1, 2)))
    factors = clip_factors(square_sums, bucket_starts)
    momentum_out = momentum_rate * momentum + factors[:, None, None] * gradient
    nesterov = (factors[:, None, None] * gradient + momentum_rate * momentum_out).astype(jnp.bfloat16)
    orthogonalized = lax.map(orthogonal, nesterov)
    update_scale = math.sqrt(max(KV, D))
    update = update_scale * orthogonalized.astype(jnp.float32)
    slot_of = slot_numbers(owners)
    positions = owners * SLOTS + slot_of
    select = (jnp.arange(N_SHARD * SLOTS, dtype=jnp.int32)[:, None] == positions[None, :]).astype(jnp.float32)
    holdings = jnp.einsum('pm,mkd->pkd', select, update).astype(jnp.bfloat16)
    return (momentum_out, update, holdings)
```

```python
import functools
import math

import jax
import jax.numpy as jnp
from jax import lax
from jax.experimental import pallas as pl
from jax.experimental.pallas import tpu as pltpu
from jax.sharding import PartitionSpec as P

D = 2048
KV = 256
ITERS = 5
MATS = 12
MESH = pl.DeviceIdType.MESH
VMEM_SPEC = pl.BlockSpec(memory_space=pltpu.VMEM)
SMEM_SPEC = pl.BlockSpec(memory_space=pltpu.SMEM)
ANY_SPEC = pl.BlockSpec(memory_space=pl.ANY)
VMEM_LIMIT = 60 * 1024 * 1024

coef_a = 3.4445
coef_b = -4.775
coef_c = 2.0315
momentum_rate = 0.95
clip_level = 0.5
epsilon = 1e-06


def orthogonal_batch(matrices):
    values = matrices.astype(jnp.float32)
    frobenius = jnp.sqrt(jnp.sum(values * values, axis=(1, 2), keepdims=True))
    matrix = (values / (frobenius + epsilon)).astype(jnp.bfloat16)
    for iteration in range(ITERS):
        gram_matrix = jnp.einsum(
            "skd,sjd->skj", matrix, matrix, preferred_element_type=jnp.float32
        ).astype(jnp.bfloat16)
        square = jnp.einsum(
            "skj,sji->ski", gram_matrix, gram_matrix, preferred_element_type=jnp.float32
        )
        mixing = (coef_b * gram_matrix.astype(jnp.float32) + coef_c * square).astype(jnp.bfloat16)
        product = jnp.einsum("skj,sjd->skd", mixing, matrix, preferred_element_type=jnp.float32)
        matrix = (coef_a * matrix.astype(jnp.float32) + product).astype(jnp.bfloat16)
    return matrix


def clip_factors(square_sums, bucket_starts):
    indices = jnp.arange(MATS, dtype=jnp.int32)
    buckets = jnp.sum((indices[:, None] >= bucket_starts[None, :]).astype(jnp.int32), axis=1)
    together = (buckets[:, None] == buckets[None, :]).astype(jnp.float32)
    totals = jnp.sum(together * square_sums[None, :], axis=1)
    members = jnp.sum(together, axis=1)
    root_mean = jnp.sqrt(totals / (members * KV * D) + epsilon)
    return jnp.minimum(1.0, clip_level / root_mean)


def slot_numbers(owners):
    indices = jnp.arange(MATS, dtype=jnp.int32)
    earlier = (indices[None, :] < indices[:, None]) & (owners[None, :] == owners[:, None])
    return jnp.sum(earlier.astype(jnp.int32), axis=1)


def selector(owner_of, slot_of, shard_count, slot_count):
    holders = lax.broadcasted_iota(jnp.int32, (shard_count, slot_count, 1), 0)
    places = lax.broadcasted_iota(jnp.int32, (shard_count, slot_count, 1), 1)
    chosen = (holders == owner_of[None, None, :]) & (places == slot_of[None, None, :])
    return chosen.astype(jnp.bfloat16)


def pack_slots(shards, chooser):
    return jnp.einsum("psm,mkd->skpd", chooser, shards, preferred_element_type=jnp.float32).astype(
        jnp.bfloat16
    )


def unpack_slots(received, chooser):
    return jnp.einsum("psm,skpd->mkd", chooser, received, preferred_element_type=jnp.float32)


def per_device_general(activations, cotangents, momentum, owners, bucket_starts):
    shard_count = lax.axis_size("shard")
    replica_count = lax.axis_size("rep")
    layers, tok_rows, width = activations.shape
    token_total = tok_rows * shard_count * replica_count
    columns = width // shard_count
    slot_count = -(-MATS // shard_count) + 1
    update_scale = math.sqrt(max(KV, D))
    partial_terms = jnp.einsum(
        "ltk,ltd->lkd", cotangents, activations, preferred_element_type=jnp.float32
    ).reshape(MATS, KV, width)
    shard_part = lax.psum_scatter(
        partial_terms.astype(jnp.bfloat16), "shard", scatter_dimension=2, tiled=True
    )
    summed = lax.psum(shard_part, "rep").astype(jnp.float32)
    gradient = summed / jnp.sqrt(jnp.float32(token_total))
    square_sums = lax.psum(jnp.sum(gradient * gradient, axis=(1, 2)), "shard")
    factors = clip_factors(square_sums, bucket_starts)
    momentum_out = momentum_rate * momentum + factors[:, None, None] * gradient
    nesterov = (factors[:, None, None] * gradient + momentum_rate * momentum_out).astype(
        jnp.bfloat16
    )
    slot_of = slot_numbers(owners)
    chooser = selector(owners, slot_of, shard_count, slot_count)
    received = lax.all_to_all(
        pack_slots(nesterov, chooser), "shard", split_axis=2, concat_axis=2, tiled=True
    )
    item_count = received.shape[0]
    result = orthogonal_batch(received.reshape(item_count, KV, width))
    scaled = (update_scale * result.astype(jnp.float32)).astype(jnp.bfloat16)
    returned_part = lax.all_to_all(
        result.reshape(item_count, KV, shard_count, columns),
        "shard",
        split_axis=2,
        concat_axis=2,
        tiled=True,
    )
    update = update_scale * unpack_slots(returned_part, chooser)
    return (momentum_out, update, scaled)


def place():
    me = lax.axis_index("rep")
    core = lax.rem(me, 2)
    x = lax.rem(lax.div(me, 2), 2)
    y = lax.div(me, 4)
    to_core = me + 1 - 2 * core
    to_x = me + 2 - 4 * x
    to_y = me + 4 - 8 * y
    to_xy = me + 6 - 4 * x - 8 * y
    return me, core, x, y, to_core, to_x, to_y, to_xy


def greet(peers):
    barrier = pltpu.get_barrier_semaphore()
    for peer in peers:
        pl.semaphore_signal(barrier, inc=1, device_id=peer, device_id_type=MESH)
    pl.semaphore_wait(barrier, len(peers))


def remote(src, dst, send, recv, peer):
    return pltpu.make_async_remote_copy(
        src_ref=src, dst_ref=dst, send_sem=send, recv_sem=recv, device_id=peer, device_id_type=MESH
    )


def plane_gather_start(z, buf_at, send, recv):
    me, core, x, y, to_core, to_x, to_y, to_xy = place()
    copies = []
    for k, peer in enumerate((to_x, to_y, to_xy, to_core)):
        c = remote(buf_at(me), buf_at(me), send.at[k], recv.at[k], (peer, z))
        c.start()
        copies.append(c)
    return copies


def plane_gather_finish(z, buf_at, send, recv, copies):
    me, core, x, y, to_core, to_x, to_y, to_xy = place()
    for k, source in enumerate((to_x, to_y, to_xy)):
        copies[k].wait_recv()
        c = remote(buf_at(source), buf_at(source), send.at[4 + k], recv.at[4 + k], (to_core, z))
        c.start()
        copies.append(c)
    for k in range(3, 7):
        copies[k].wait_recv()
    for c in copies:
        c.wait_send()


def reduce_kernel(
    n_shard, inverse, lay_ref, half_ref, act_ref, cot_ref, gall_ref, sq_ref,
    act, cot, part, recv1, turn, recv2, plane, zrecv,
    local_sem, in_send, in_recv, s1, r1, s2, r2, s3, r3, gs, gr, qs, qr,
):
    me, core, x, y, to_core, to_x, to_y, to_xy = place()
    z = lax.axis_index("shard")
    tokens = act_ref.shape[1]
    rows, cols = part.shape[-2:]
    members = part.shape[2 + 1]
    steps = [d for d in (2, 1, 3) if d < n_shard] + list(range(4, n_shard)) + [0]
    peers = [(p, z) for p in (to_core, to_x, to_y, to_xy)]
    peers += [(me, lax.rem(z + d, n_shard)) for d in range(1, n_shard)]
    own = [
        pltpu.make_async_copy(act_ref, act.at[:, pl.ds(0, tokens)], local_sem.at[0]),
        pltpu.make_async_copy(cot_ref, cot.at[:, pl.ds(0, tokens)], local_sem.at[1]),
    ]
    for c in own:
        c.start()
    greet(peers)
    swap = [
        remote(cot_ref, cot.at[:, pl.ds(tokens, tokens)], in_send.at[1], in_recv.at[1], (to_core, z)),
        remote(act_ref, act.at[:, pl.ds(tokens, tokens)], in_send.at[0], in_recv.at[0], (to_core, z)),
    ]
    for c in swap:
        c.start()
    for c in own:
        c.wait()
    for c in swap:
        c.wait()
    first = []
    for k, d in enumerate(steps):
        offset = pl.multiple_of(lax.rem(z + d, n_shard) * cols, cols)

        def one(q, carry, k=k, offset=offset):
            group = lax.div(q, members)
            member = lax.rem(q, members)
            block = cot[lay_ref[q]]
            low = jnp.where(core == 0, block[:, :rows], block[:, rows : 2 * rows])
            high = jnp.where(core == 0, block[:, 2 * rows : 3 * rows], block[:, 3 * rows :])
            left = jnp.where(half_ref[q] == 0, low, high)
            right = act[lay_ref[q], :, pl.ds(offset, cols)]
            value = lax.dot_general(
                left, right, (((0,), (0,)), ((), ())), preferred_element_type=jnp.float32
            )
            part[k, lax.div(group, 2), lax.rem(group, 2), member] = value.astype(part.dtype)
            return carry

        lax.fori_loop(0, 4 * members, one, 0)
        if k % 2 == 0:
            c = remote(part.at[k, :, 1 - x], recv1.at[k], s1.at[k], r1.at[k], (to_x, z))
        else:
            c = remote(part.at[k, 1 - y], recv1.at[k], s1.at[k], r1.at[k], (to_y, z))
        c.start()
        first.append(c)
    second = []
    for k in range(n_shard):
        first[k].wait_recv()

        def add_out(j, carry, k=k):
            if k % 2 == 0:
                mine = part[k, 1 - y, x, j]
                came = recv1[k, 1 - y, j]
            else:
                mine = part[k, y, 1 - x, j]
                came = recv1[k, 1 - x, j]
            turn[k, j] = (mine.astype(jnp.float32) + came.astype(jnp.float32)).astype(turn.dtype)
            return carry

        lax.fori_loop(0, members, add_out, 0)
        c = remote(
            turn.at[k], recv2.at[k], s2.at[k], r2.at[k], (to_y if k % 2 == 0 else to_x, z)
        )
        c.start()
        second.append(c)
    third = []
    for k, d in enumerate(steps):
        second[k].wait_recv()

        def add_in(j, carry, k=k):
            came = recv1[k, y, j] if k % 2 == 0 else recv1[k, x, j]
            value = part[k, y, x, j].astype(jnp.float32) + came.astype(jnp.float32)
            value = value + recv2[k, j].astype(jnp.float32)
            plane[k, j] = value.astype(plane.dtype)
            return carry

        lax.fori_loop(0, members, add_in, 0)
        if d:
            c = remote(
                plane.at[k], zrecv.at[k], s3.at[k], r3.at[k], (me, lax.rem(z + d, n_shard))
            )
            c.start()
            third.append(c)
    for c in third:
        c.wait_recv()

    def add_last(j, carry):
        value = plane[n_shard - 1, j].astype(jnp.float32)
        for k in range(n_shard - 1):
            value = value + zrecv[k, j].astype(jnp.float32)
        gall_ref[me, j] = (value * inverse).astype(gall_ref.dtype)
        return carry

    lax.fori_loop(0, members, add_last, 0)
    at = lambda r: gall_ref.at[r]
    copies = plane_gather_start(z, at, gs, gr)
    plane_gather_finish(z, at, gs, gr, copies)

    def square(r, carry):
        for j in range(members):
            value = gall_ref[r, j].astype(jnp.float32)
            sq_ref[0, r, j] = jnp.sum(value * value, axis=0, keepdims=True)
        return carry

    lax.fori_loop(0, gall_ref.shape[0], square, 0)
    fourth = []
    for d in range(1, n_shard):
        c = remote(
            sq_ref.at[0], sq_ref.at[d], qs.at[d - 1], qr.at[d - 1],
            (me, lax.rem(z + d, n_shard)),
        )
        c.start()
        fourth.append(c)
    for c in fourth:
        c.wait()
    for c in first + second + third:
        c.wait_send()


def momentum_kernel(perm_ref, factor_ref, momentum_ref, grad_ref, out_ref, u_ref):
    q = pl.program_id(0)
    factor = factor_ref[perm_ref[q]]
    rows = grad_ref.shape[3]
    for c in range(2):
        cut = pl.ds(c * rows, rows)
        step = factor * grad_ref[0, c, 0].astype(jnp.float32)
        new = momentum_rate * momentum_ref[0, cut] + step
        out_ref[0, cut] = new
        u_ref[0, 0, cut] = (step + momentum_rate * new).astype(u_ref.dtype)


def spread_kernel(n_shard, u_ref, full_ref, local_sem, zs, zr, cs, cr):
    me, core, x, y, to_core, to_x, to_y, to_xy = place()
    z = lax.axis_index("shard")
    group = lax.div(me, 2)
    rows = full_ref.shape[1] // 2
    cols = full_ref.shape[2] // n_shard

    def at(shard):
        return full_ref.at[
            :, pl.ds(pl.multiple_of(core * rows, rows), rows),
            pl.ds(pl.multiple_of(shard * cols, cols), cols),
        ]

    local = pltpu.make_async_copy(
        u_ref.at[group], full_ref.at[:, :, pl.ds(pl.multiple_of(z * cols, cols), cols)], local_sem
    )
    local.start()
    greet([(to_core, z)] + [(me, lax.rem(z + d, n_shard)) for d in range(1, n_shard)])
    mine = u_ref.at[group, :, pl.ds(pl.multiple_of(core * rows, rows), rows)]
    order = [d for d in (2, 1, 3) if d < n_shard] + list(range(4, n_shard))
    copies = []
    for d in order:
        c = remote(mine, at(z), zs.at[d - 1], zr.at[d - 1], (me, lax.rem(z + d, n_shard)))
        c.start()
        copies.append(c)
    onward = []
    for c, d in zip(copies, order):
        c.wait_recv()
        source = lax.rem(z + n_shard - d, n_shard)
        f = remote(at(source), at(source), cs.at[d - 1], cr.at[d - 1], (to_core, z))
        f.start()
        onward.append(f)
    for f in onward:
        f.wait_recv()
    for c in copies + onward:
        c.wait_send()
    local.wait()


def newton_kernel(u_ref, o_ref):
    def total(i, carry):
        value = u_ref[0, pl.ds(pl.multiple_of(i * 32, 32), 32), :].astype(jnp.float32)
        return carry + jnp.sum(value * value, axis=0, keepdims=True)

    kv, width = u_ref.shape[1:]
    sums = lax.fori_loop(0, kv // 32, total, jnp.zeros((1, width), jnp.float32))
    inverse = 1.0 / (jnp.sqrt(jnp.sum(sums, axis=1, keepdims=True)) + epsilon)
    matrix = (u_ref[0].astype(jnp.float32) * inverse).astype(jnp.bfloat16)
    for iteration in range(ITERS):
        gram = lax.dot_general(
            matrix, matrix, (((1,), (1,)), ((), ())), preferred_element_type=jnp.float32
        ).astype(jnp.bfloat16)
        square = jnp.dot(gram, gram, preferred_element_type=jnp.float32)
        mixing = (coef_b * gram.astype(jnp.float32) + coef_c * square).astype(jnp.bfloat16)
        product = jnp.dot(mixing, matrix, preferred_element_type=jnp.float32)
        matrix = (coef_a * matrix.astype(jnp.float32) + product).astype(jnp.bfloat16)
    o_ref[0] = matrix


def share_kernel(
    n_shard, pick_ref, keep_ref, o_ref, oall_ref, whole_ref, us, ur, ws, wr
):
    me, core, x, y, to_core, to_x, to_y, to_xy = place()
    z = lax.axis_index("shard")
    group = lax.div(me, 2)
    rows = o_ref.shape[1] // 2
    cols = o_ref.shape[2] // n_shard
    half = pl.ds(pl.multiple_of(core * rows, rows), rows)
    for j in range(o_ref.shape[0]):
        oall_ref[me, j] = o_ref[j, half, pl.ds(pl.multiple_of(z * cols, cols), cols)]
    chosen = o_ref[pick_ref[0], half, :]
    whole_ref[me] = (chosen.astype(jnp.float32) * keep_ref[0]).astype(whole_ref.dtype)
    greet([(p, z) for p in (to_core, to_x, to_y, to_xy)])
    at_u = lambda r: oall_ref.at[r]
    at_w = lambda r: whole_ref.at[r]
    cu = plane_gather_start(z, at_u, us, ur)
    cw = plane_gather_start(z, at_w, ws, wr)
    plane_gather_finish(z, at_u, us, ur, cu)
    plane_gather_finish(z, at_w, ws, wr, cw)


def update_kernel(scale, perm_ref, o_ref, out_ref):
    rows = o_ref.shape[3]
    for c in range(2):
        out_ref[0, pl.ds(c * rows, rows)] = scale * o_ref[0, c, 0].astype(jnp.float32)


def owned_kernel(scale, index_ref, keep_ref, w_ref, out_ref):
    rows = w_ref.shape[2]
    keep = keep_ref[pl.program_id(0)]
    for c in range(2):
        value = scale * w_ref[0, c].astype(jnp.float32)
        out_ref[0, pl.ds(c * rows, rows)] = (value * keep).astype(out_ref.dtype)


def per_device_planes(activations, cotangents, momentum, owners, bucket_starts):
    n_shard = lax.axis_size("shard")
    n_rep = lax.axis_size("rep")
    layers, tok_rows, width = activations.shape
    token_total = tok_rows * n_shard * n_rep
    cols = width // n_shard
    rows = KV // 2
    groups = n_rep // 2
    members = MATS // groups
    slots = -(-MATS // n_shard) + 1
    update_scale = math.sqrt(max(KV, D))
    bf16, f32, i32 = jnp.bfloat16, jnp.float32, jnp.int32
    z = lax.axis_index("shard")
    my_group = lax.axis_index("rep") // 2

    index = jnp.arange(MATS, dtype=i32)
    before = (owners[None, :] < owners[:, None]) | (
        (owners[None, :] == owners[:, None]) & (index[None, :] < index[:, None])
    )
    rank = jnp.sum(before.astype(i32), axis=1)
    position = (rank % groups) * members + rank // groups
    perm = jnp.sum(jnp.where(position[None, :] == index[:, None], index[None, :], 0), axis=1)
    start = jnp.sum((owners < z).astype(i32))
    count = jnp.sum((owners == z).astype(i32))

    params = functools.partial(
        pltpu.CompilerParams, has_side_effects=True, vmem_limit_bytes=VMEM_LIMIT
    )
    dma = pltpu.SemaphoreType.DMA
    gall, sq = pl.pallas_call(
        functools.partial(reduce_kernel, n_shard, 1.0 / math.sqrt(token_total)),
        out_shape=(
            jax.ShapeDtypeStruct((n_rep, members, rows, cols), bf16),
            jax.ShapeDtypeStruct((n_shard, n_rep, members, 1, cols), f32),
        ),
        in_specs=[SMEM_SPEC, SMEM_SPEC, ANY_SPEC, ANY_SPEC],
        out_specs=(VMEM_SPEC, VMEM_SPEC),
        scratch_shapes=[
            pltpu.VMEM((layers, 2 * tok_rows, width), bf16),
            pltpu.VMEM((layers, 2 * tok_rows, 2 * KV), bf16),
            pltpu.VMEM((n_shard, 2, 2, members, rows, cols), bf16),
            pltpu.VMEM((n_shard, 2, members, rows, cols), bf16),
            pltpu.VMEM((n_shard, members, rows, cols), bf16),
            pltpu.VMEM((n_shard, members, rows, cols), bf16),
            pltpu.VMEM((n_shard, members, rows, cols), bf16),
            pltpu.VMEM((n_shard - 1, members, rows, cols), bf16),
            dma((2,)), dma((2,)), dma((2,)),
            dma((n_shard,)), dma((n_shard,)), dma((n_shard,)), dma((n_shard,)),
            dma((n_shard,)), dma((n_shard,)),
            dma((7,)), dma((7,)), dma((n_shard - 1,)), dma((n_shard - 1,)),
        ],
        compiler_params=params(collective_id=0),
        name="reduce",
    )(perm // 2, perm % 2, activations, cotangents)

    by_position = jnp.sum(
        sq.reshape(n_shard, groups, 2, members, cols), axis=(0, 2, 4)
    ).reshape(MATS)
    square_sums = jnp.sum(
        jnp.where(position[:, None] == index[None, :], by_position[None, :], 0.0), axis=1
    )
    factors = clip_factors(square_sums, bucket_starts)

    momentum_out, nesterov = pl.pallas_call(
        momentum_kernel,
        out_shape=(
            jax.ShapeDtypeStruct(momentum.shape, f32),
            jax.ShapeDtypeStruct((groups, members, KV, cols), bf16),
        ),
        grid_spec=pltpu.PrefetchScalarGridSpec(
            num_scalar_prefetch=2,
            grid=(MATS,),
            in_specs=[
                pl.BlockSpec((1, KV, cols), lambda q, p, f: (p[q], 0, 0)),
                pl.BlockSpec(
                    (1, 2, 1, rows, cols), lambda q, p, f: (q // members, 0, q % members, 0, 0)
                ),
            ],
            out_specs=(
                pl.BlockSpec((1, KV, cols), lambda q, p, f: (p[q], 0, 0)),
                pl.BlockSpec((1, 1, KV, cols), lambda q, p, f: (q // members, q % members, 0, 0)),
            ),
        ),
        name="momentum",
    )(perm, factors, momentum, gall.reshape(groups, 2, members, rows, cols))

    full = pl.pallas_call(
        functools.partial(spread_kernel, n_shard),
        out_shape=jax.ShapeDtypeStruct((members, KV, width), bf16),
        in_specs=[ANY_SPEC],
        out_specs=VMEM_SPEC,
        scratch_shapes=[dma(())] + [dma((n_shard - 1,)) for _ in range(4)],
        compiler_params=params(collective_id=1),
        name="spread",
    )(nesterov)

    result = pl.pallas_call(
        newton_kernel,
        out_shape=jax.ShapeDtypeStruct((members, KV, width), bf16),
        grid=(members,),
        in_specs=[pl.BlockSpec((1, KV, width), lambda i: (i, 0, 0))],
        out_specs=pl.BlockSpec((1, KV, width), lambda i: (i, 0, 0)),
        name="newton",
    )(full)

    mine = start + (my_group - start) % groups
    keep = (mine < start + count).astype(f32)
    pick = jnp.minimum(mine // groups, members - 1)
    oall, whole = pl.pallas_call(
        functools.partial(share_kernel, n_shard),
        out_shape=(
            jax.ShapeDtypeStruct((n_rep, members, rows, cols), bf16),
            jax.ShapeDtypeStruct((n_rep, rows, width), bf16),
        ),
        in_specs=[SMEM_SPEC, SMEM_SPEC, VMEM_SPEC],
        out_specs=(VMEM_SPEC, VMEM_SPEC),
        scratch_shapes=[dma((7,)) for _ in range(4)],
        compiler_params=params(collective_id=2),
        name="share",
    )(pick.reshape(1), keep.reshape(1), result)

    update = pl.pallas_call(
        functools.partial(update_kernel, update_scale),
        out_shape=jax.ShapeDtypeStruct(momentum.shape, f32),
        grid_spec=pltpu.PrefetchScalarGridSpec(
            num_scalar_prefetch=1,
            grid=(MATS,),
            in_specs=[
                pl.BlockSpec(
                    (1, 2, 1, rows, cols), lambda q, p: (q // members, 0, q % members, 0, 0)
                )
            ],
            out_specs=pl.BlockSpec((1, KV, cols), lambda q, p: (p[q], 0, 0)),
        ),
        name="update",
    )(perm, oall.reshape(groups, 2, members, rows, cols))

    slot = jnp.arange(slots, dtype=i32)
    owned = pl.pallas_call(
        functools.partial(owned_kernel, update_scale),
        out_shape=jax.ShapeDtypeStruct((slots, KV, width), bf16),
        grid_spec=pltpu.PrefetchScalarGridSpec(
            num_scalar_prefetch=2,
            grid=(slots,),
            in_specs=[pl.BlockSpec((1, 2, rows, width), lambda s, i, k: (i[s], 0, 0, 0))],
            out_specs=pl.BlockSpec((1, KV, width), lambda s, i, k: (s, 0, 0)),
        ),
        name="owned",
    )(
        (start + slot) % groups,
        (slot < count).astype(f32),
        whole.reshape(groups, 2, rows, width),
    )
    return (momentum_out, update, owned)


def solution(mesh):
    groups = mesh.shape["rep"] // 2
    slots = -(-MATS // mesh.shape["shard"]) + 1
    fits = mesh.shape["rep"] == 8 and MATS % groups == 0 and slots <= groups
    placed = (
        P(None, ("rep", "shard"), None),
        P(None, ("rep", "shard"), None),
        P(None, None, "shard"),
        P(),
        P(),
    )
    return jax.shard_map(
        per_device_planes if fits else per_device_general,
        mesh=mesh,
        in_specs=placed,
        out_specs=(P(None, None, "shard"), P(None, None, "shard"), P("shard", None, None)),
        check_vma=False,
    )
```

```python
import functools
import math

import jax
import jax.numpy as jnp
from jax import lax
from jax.experimental import pallas as pl
from jax.experimental.pallas import tpu as pltpu
from jax.sharding import PartitionSpec as P

D = 2048
KV = 256
ITERS = 5
MATS = 12
MESH = pl.DeviceIdType.MESH
VMEM_SPEC = pl.BlockSpec(memory_space=pltpu.VMEM)
SMEM_SPEC = pl.BlockSpec(memory_space=pltpu.SMEM)
ANY_SPEC = pl.BlockSpec(memory_space=pl.ANY)
VMEM_LIMIT = 60 * 1024 * 1024

coef_a = 3.4445
coef_b = -4.775
coef_c = 2.0315
momentum_rate = 0.95
clip_level = 0.5
epsilon = 1e-06


def orthogonal_batch(matrices):
    values = matrices.astype(jnp.float32)
    frobenius = jnp.sqrt(jnp.sum(values * values, axis=(1, 2), keepdims=True))
    matrix = (values / (frobenius + epsilon)).astype(jnp.bfloat16)
    for iteration in range(ITERS):
        gram_matrix = jnp.einsum(
            "skd,sjd->skj", matrix, matrix, preferred_element_type=jnp.float32
        ).astype(jnp.bfloat16)
        square = jnp.einsum(
            "skj,sji->ski", gram_matrix, gram_matrix, preferred_element_type=jnp.float32
        )
        mixing = (coef_b * gram_matrix.astype(jnp.float32) + coef_c * square).astype(jnp.bfloat16)
        product = jnp.einsum("skj,sjd->skd", mixing, matrix, preferred_element_type=jnp.float32)
        matrix = (coef_a * matrix.astype(jnp.float32) + product).astype(jnp.bfloat16)
    return matrix


def clip_factors(square_sums, bucket_starts):
    indices = jnp.arange(MATS, dtype=jnp.int32)
    buckets = jnp.sum((indices[:, None] >= bucket_starts[None, :]).astype(jnp.int32), axis=1)
    together = (buckets[:, None] == buckets[None, :]).astype(jnp.float32)
    totals = jnp.sum(together * square_sums[None, :], axis=1)
    members = jnp.sum(together, axis=1)
    root_mean = jnp.sqrt(totals / (members * KV * D) + epsilon)
    return jnp.minimum(1.0, clip_level / root_mean)


def slot_numbers(owners):
    indices = jnp.arange(MATS, dtype=jnp.int32)
    earlier = (indices[None, :] < indices[:, None]) & (owners[None, :] == owners[:, None])
    return jnp.sum(earlier.astype(jnp.int32), axis=1)


def selector(owner_of, slot_of, shard_count, slot_count):
    holders = lax.broadcasted_iota(jnp.int32, (shard_count, slot_count, 1), 0)
    places = lax.broadcasted_iota(jnp.int32, (shard_count, slot_count, 1), 1)
    chosen = (holders == owner_of[None, None, :]) & (places == slot_of[None, None, :])
    return chosen.astype(jnp.bfloat16)


def pack_slots(shards, chooser):
    return jnp.einsum("psm,mkd->skpd", chooser, shards, preferred_element_type=jnp.float32).astype(
        jnp.bfloat16
    )


def unpack_slots(received, chooser):
    return jnp.einsum("psm,skpd->mkd", chooser, received, preferred_element_type=jnp.float32)


def per_device_general(activations, cotangents, momentum, owners, bucket_starts):
    shard_count = lax.axis_size("shard")
    replica_count = lax.axis_size("rep")
    layers, tok_rows, width = activations.shape
    token_total = tok_rows * shard_count * replica_count
    columns = width // shard_count
    slot_count = -(-MATS // shard_count) + 1
    update_scale = math.sqrt(max(KV, D))
    partial_terms = jnp.einsum(
        "ltk,ltd->lkd", cotangents, activations, preferred_element_type=jnp.float32
    ).reshape(MATS, KV, width)
    shard_part = lax.psum_scatter(
        partial_terms.astype(jnp.bfloat16), "shard", scatter_dimension=2, tiled=True
    )
    summed = lax.psum(shard_part, "rep").astype(jnp.float32)
    gradient = summed / jnp.sqrt(jnp.float32(token_total))
    square_sums = lax.psum(jnp.sum(gradient * gradient, axis=(1, 2)), "shard")
    factors = clip_factors(square_sums, bucket_starts)
    momentum_out = momentum_rate * momentum + factors[:, None, None] * gradient
    nesterov = (factors[:, None, None] * gradient + momentum_rate * momentum_out).astype(
        jnp.bfloat16
    )
    slot_of = slot_numbers(owners)
    chooser = selector(owners, slot_of, shard_count, slot_count)
    received = lax.all_to_all(
        pack_slots(nesterov, chooser), "shard", split_axis=2, concat_axis=2, tiled=True
    )
    item_count = received.shape[0]
    result = orthogonal_batch(received.reshape(item_count, KV, width))
    scaled = (update_scale * result.astype(jnp.float32)).astype(jnp.bfloat16)
    returned_part = lax.all_to_all(
        result.reshape(item_count, KV, shard_count, columns),
        "shard",
        split_axis=2,
        concat_axis=2,
        tiled=True,
    )
    update = update_scale * unpack_slots(returned_part, chooser)
    return (momentum_out, update, scaled)


def place():
    me = lax.axis_index("rep")
    core = lax.rem(me, 2)
    x = lax.rem(lax.div(me, 2), 2)
    y = lax.div(me, 4)
    to_core = me + 1 - 2 * core
    to_x = me + 2 - 4 * x
    to_y = me + 4 - 8 * y
    to_xy = me + 6 - 4 * x - 8 * y
    return me, core, x, y, to_core, to_x, to_y, to_xy


def greet(peers):
    barrier = pltpu.get_barrier_semaphore()
    for peer in peers:
        pl.semaphore_signal(barrier, inc=1, device_id=peer, device_id_type=MESH)
    pl.semaphore_wait(barrier, len(peers))


def remote(src, dst, send, recv, peer):
    return pltpu.make_async_remote_copy(
        src_ref=src, dst_ref=dst, send_sem=send, recv_sem=recv, device_id=peer, device_id_type=MESH
    )


def plane_gather_start(z, at, send, recv):
    me, core, x, y, to_core, to_x, to_y, to_xy = place()
    plan = ((0, to_x, 0), (2, to_y, 1), (1, to_x, 1), (3, to_y, 0), (4, to_core, None))
    copies = {}
    for k, peer, half in plan:
        copies[k] = remote(at(me, half), at(me, half), send.at[k], recv.at[k], (peer, z))
        copies[k].start()
    return copies


def plane_gather_turn(z, at, send, recv, copies):
    me, core, x, y, to_core, to_x, to_y, to_xy = place()

    def forward(k, block, half, peer):
        copies[k] = remote(
            at(block, half), at(block, half), send.at[k], recv.at[k], (peer, z)
        )
        copies[k].start()

    copies[0].wait_recv()
    forward(5, to_x, 0, to_y)
    copies[2].wait_recv()
    forward(6, to_y, 1, to_x)
    copies[1].wait_recv()
    forward(7, to_x, None, to_core)
    copies[3].wait_recv()
    forward(8, to_y, None, to_core)


def plane_gather_finish(z, at, send, recv, copies):
    me, core, x, y, to_core, to_x, to_y, to_xy = place()
    copies[5].wait_recv()
    copies[6].wait_recv()
    copies[9] = remote(
        at(to_xy, None), at(to_xy, None), send.at[9], recv.at[9], (to_core, z)
    )
    copies[9].start()
    for k in (4, 7, 8, 9):
        copies[k].wait_recv()
    for k in range(10):
        copies[k].wait_send()


def block_at(ref, axis):
    rows = ref.shape[axis] // 2

    def at(r, half):
        if half is None:
            return ref.at[r]
        cut = pl.ds(half * rows, rows)
        return ref.at[r, cut] if axis == 1 else ref.at[r, :, cut]

    return at


def reduce_kernel(
    n_shard, inverse, lay_ref, half_ref, act_ref, cot_ref, gall_ref, sq_ref,
    act, cot, part, recv1, turn, recv2, plane, zrecv,
    local_sem, in_send, in_recv, s1, r1, s2, r2, s3, r3, gs, gr, qs, qr,
):
    me, core, x, y, to_core, to_x, to_y, to_xy = place()
    z = lax.axis_index("shard")
    tokens = act_ref.shape[1]
    rows, cols = part.shape[-2:]
    members = part.shape[2 + 1]
    steps = [d for d in (2, 1, 3) if d < n_shard] + list(range(4, n_shard)) + [0]
    peers = [(p, z) for p in (to_core, to_x, to_y, to_xy)]
    peers += [(me, lax.rem(z + d, n_shard)) for d in range(1, n_shard)]
    own = [
        pltpu.make_async_copy(act_ref, act.at[:, pl.ds(0, tokens)], local_sem.at[0]),
        pltpu.make_async_copy(cot_ref, cot.at[:, pl.ds(0, tokens)], local_sem.at[1]),
    ]
    for c in own:
        c.start()
    greet(peers)
    swap = [
        remote(cot_ref, cot.at[:, pl.ds(tokens, tokens)], in_send.at[1], in_recv.at[1], (to_core, z)),
        remote(act_ref, act.at[:, pl.ds(tokens, tokens)], in_send.at[0], in_recv.at[0], (to_core, z)),
    ]
    for c in swap:
        c.start()
    for c in own:
        c.wait()
    for c in swap:
        c.wait()
    first = []
    second = []
    third = []

    def launch(k):
        offset = pl.multiple_of(lax.rem(z + steps[k], n_shard) * cols, cols)

        def one(q, carry):
            group = lax.div(q, members)
            member = lax.rem(q, members)
            block = cot[lay_ref[q]]
            low = jnp.where(core == 0, block[:, :rows], block[:, rows : 2 * rows])
            high = jnp.where(core == 0, block[:, 2 * rows : 3 * rows], block[:, 3 * rows :])
            left = jnp.where(half_ref[q] == 0, low, high)
            right = act[lay_ref[q], :, pl.ds(offset, cols)]
            value = lax.dot_general(
                left, right, (((0,), (0,)), ((), ())), preferred_element_type=jnp.float32
            )
            part[k, lax.div(group, 2), lax.rem(group, 2), member] = value.astype(part.dtype)
            return carry

        lax.fori_loop(0, 4 * members, one, 0)

    def send_first(k):
        if k % 2 == 0:
            c = remote(part.at[k, :, 1 - x], recv1.at[k], s1.at[k], r1.at[k], (to_x, z))
        else:
            c = remote(part.at[k, 1 - y], recv1.at[k], s1.at[k], r1.at[k], (to_y, z))
        c.start()
        first.append(c)

    def send_second(k):
        first[k].wait_recv()

        def add_out(j, carry):
            if k % 2 == 0:
                mine = part[k, 1 - y, x, j]
                came = recv1[k, 1 - y, j]
            else:
                mine = part[k, y, 1 - x, j]
                came = recv1[k, 1 - x, j]
            turn[k, j] = (mine.astype(jnp.float32) + came.astype(jnp.float32)).astype(turn.dtype)
            return carry

        lax.fori_loop(0, members, add_out, 0)
        c = remote(
            turn.at[k], recv2.at[k], s2.at[k], r2.at[k], (to_y if k % 2 == 0 else to_x, z)
        )
        c.start()
        second.append(c)

    def send_third(k):
        second[k].wait_recv()

        def add_in(j, carry):
            came = recv1[k, y, j] if k % 2 == 0 else recv1[k, x, j]
            value = part[k, y, x, j].astype(jnp.float32) + came.astype(jnp.float32)
            value = value + recv2[k, j].astype(jnp.float32)
            plane[k, j] = value.astype(plane.dtype)
            return carry

        lax.fori_loop(0, members, add_in, 0)
        if steps[k]:
            c = remote(
                plane.at[k], zrecv.at[k], s3.at[k], r3.at[k],
                (me, lax.rem(z + steps[k], n_shard)),
            )
            c.start()
            third.append(c)

    launch(0)
    send_first(0)
    launch(1)
    send_first(1)
    for k in range(2, n_shard):
        launch(k)
    for k in range(0, n_shard, 2):
        pair = [i for i in (k, k + 1) if i < n_shard]
        for i in pair:
            send_second(i)
        for i in (k + 2, k + 3):
            if i < n_shard:
                send_first(i)
        for i in pair:
            send_third(i)
    for c in third:
        c.wait_recv()

    def add_last(j, carry):
        value = plane[n_shard - 1, j].astype(jnp.float32)
        for k in range(n_shard - 1):
            value = value + zrecv[k, j].astype(jnp.float32)
        gall_ref[me, j] = (value * inverse).astype(gall_ref.dtype)
        return carry

    lax.fori_loop(0, members, add_last, 0)
    at = block_at(gall_ref, 2)
    copies = plane_gather_start(z, at, gs, gr)
    plane_gather_turn(z, at, gs, gr, copies)
    plane_gather_finish(z, at, gs, gr, copies)

    def square(r, carry):
        for j in range(members):
            value = gall_ref[r, j].astype(jnp.float32)
            sq_ref[0, r, j] = jnp.sum(value * value, axis=0, keepdims=True)
        return carry

    lax.fori_loop(0, gall_ref.shape[0], square, 0)
    fourth = []
    for d in range(1, n_shard):
        c = remote(
            sq_ref.at[0], sq_ref.at[d], qs.at[d - 1], qr.at[d - 1],
            (me, lax.rem(z + d, n_shard)),
        )
        c.start()
        fourth.append(c)
    for c in fourth:
        c.wait()
    for c in first + second + third:
        c.wait_send()


def spread_kernel(
    n_shard, mat_ref, place_ref, factor_ref, momentum_ref, gall_ref, full_ref,
    held, zs, zr, cs, cr,
):
    me, core, x, y, to_core, to_x, to_y, to_xy = place()
    z = lax.axis_index("shard")
    block = me - core
    rows = full_ref.shape[0] // 2
    cols = full_ref.shape[1] // n_shard

    def at(side, shard):
        return (
            pl.ds(pl.multiple_of(side * rows, rows), rows),
            pl.ds(pl.multiple_of(shard * cols, cols), cols),
        )

    def nesterov(p, side):
        matrix = mat_ref[p]
        half = pl.ds(pl.multiple_of(side * rows, rows), rows)
        step = factor_ref[matrix] * gall_ref[block + side, place_ref[p]].astype(jnp.float32)
        new = momentum_rate * momentum_ref[matrix, half] + step
        return (step + momentum_rate * new).astype(full_ref.dtype)

    order = [d for d in (2, 1, 3) if d < n_shard] + list(range(4, n_shard))
    for d in order:
        held[d - 1] = nesterov(lax.rem(z + d, n_shard), core)
    greet([(to_core, z)] + [(me, lax.rem(z + d, n_shard)) for d in range(1, n_shard)])
    copies = []
    for d in order:
        peer = (me, lax.rem(z + d, n_shard))
        c = remote(held.at[d - 1], full_ref.at[at(core, z)], zs.at[d - 1], zr.at[d - 1], peer)
        c.start()
        copies.append(c)
    for side in range(2):
        full_ref[at(side, z)] = nesterov(z, side)
    onward = []
    for c, d in zip(copies, order):
        c.wait_recv()
        source = full_ref.at[at(core, lax.rem(z + n_shard - d, n_shard))]
        f = remote(source, source, cs.at[d - 1], cr.at[d - 1], (to_core, z))
        f.start()
        onward.append(f)
    for f in onward:
        f.wait_recv()
    for c in copies + onward:
        c.wait_send()


def newton_kernel(u_ref, o_ref):
    def total(i, carry):
        value = u_ref[pl.ds(pl.multiple_of(i * 32, 32), 32), :].astype(jnp.float32)
        return carry + jnp.sum(value * value, axis=0, keepdims=True)

    kv, width = u_ref.shape
    sums = lax.fori_loop(0, kv // 32, total, jnp.zeros((1, width), jnp.float32))
    inverse = 1.0 / (jnp.sqrt(jnp.sum(sums, axis=1, keepdims=True)) + epsilon)
    matrix = (u_ref[...].astype(jnp.float32) * inverse).astype(jnp.bfloat16)
    for iteration in range(ITERS):
        gram = lax.dot_general(
            matrix, matrix, (((1,), (1,)), ((), ())), preferred_element_type=jnp.float32
        ).astype(jnp.bfloat16)
        square = jnp.dot(gram, gram, preferred_element_type=jnp.float32)
        mixing = (coef_b * gram.astype(jnp.float32) + coef_c * square).astype(jnp.bfloat16)
        product = jnp.dot(mixing, matrix, preferred_element_type=jnp.float32)
        matrix = (coef_a * matrix.astype(jnp.float32) + product).astype(jnp.bfloat16)
    o_ref[...] = matrix


def share_kernel(
    n_shard, owner_ref, o_ref, oall_ref, whole_ref, back, bs, br, us, ur, ws, wr
):
    me, core, x, y, to_core, to_x, to_y, to_xy = place()
    z = lax.axis_index("shard")
    rows = o_ref.shape[0] // 2
    cols = o_ref.shape[1] // n_shard
    half = pl.ds(pl.multiple_of(core * rows, rows), rows)

    def piece(shard):
        return half, pl.ds(pl.multiple_of(shard * cols, cols), cols)

    peers = [(p, z) for p in (to_core, to_x, to_y)]
    peers += [(me, lax.rem(z + d, n_shard)) for d in range(1, n_shard)]
    greet(peers)
    order = [d for d in (2, 1, 3) if d < n_shard] + list(range(4, n_shard))
    returns = []
    for d in order:
        to = lax.rem(z + d, n_shard)
        c = remote(o_ref.at[piece(to)], back.at[z], bs.at[d - 1], br.at[d - 1], (me, to))
        c.start()
        returns.append(c)
    whole_ref[me] = o_ref[half]
    at_w = block_at(whole_ref, 1)
    at_u = block_at(oall_ref, 2)
    cw = plane_gather_start(z, at_w, ws, wr)
    back[z] = o_ref[piece(z)]
    for c in returns:
        c.wait_recv()
    for j in range(oall_ref.shape[1]):
        oall_ref[me, j] = back[owner_ref[j]]
    cu = plane_gather_start(z, at_u, us, ur)
    plane_gather_turn(z, at_w, ws, wr, cw)
    plane_gather_turn(z, at_u, us, ur, cu)
    plane_gather_finish(z, at_w, ws, wr, cw)
    plane_gather_finish(z, at_u, us, ur, cu)
    for c in returns:
        c.wait_send()


def finish_kernel(
    scale, block_ref, member_ref, factor_ref, slot_ref, keep_ref,
    gall_ref, oall_ref, whole_ref, momentum_ref, mout_ref, update_ref, owned_ref,
    mbuf, ubuf, wbuf, load, msem, usem, wsem,
):
    mats = mbuf.shape[0]
    slots = wbuf.shape[0]
    rows = gall_ref.shape[2]

    def fetch(m):
        return pltpu.make_async_copy(momentum_ref.at[m], mbuf.at[m], load.at[m])

    def put(buf, out, sem, m):
        return pltpu.make_async_copy(buf.at[m], out.at[m], sem.at[m])

    def each(count, body):
        def step(m, carry):
            body(m)
            return carry

        lax.fori_loop(0, count, step, 0)

    each(mats, lambda m: fetch(m).start())

    def owned_one(s):
        for c in range(2):
            value = scale * whole_ref[slot_ref[s] + c].astype(jnp.float32)
            wbuf[s, pl.ds(c * rows, rows)] = (value * keep_ref[s]).astype(wbuf.dtype)
        put(wbuf, owned_ref, wsem, s).start()

    def update_one(m):
        for c in range(2):
            value = oall_ref[block_ref[m] + c, member_ref[m]].astype(jnp.float32)
            ubuf[m, pl.ds(c * rows, rows)] = scale * value
        put(ubuf, update_ref, usem, m).start()

    def momentum_one(m):
        fetch(m).wait()
        for c in range(2):
            cut = pl.ds(c * rows, rows)
            step = factor_ref[m] * gall_ref[block_ref[m] + c, member_ref[m]].astype(jnp.float32)
            mbuf[m, cut] = momentum_rate * mbuf[m, cut] + step
        put(mbuf, mout_ref, msem, m).start()

    each(slots, owned_one)
    each(mats, update_one)
    each(mats, momentum_one)
    each(slots, lambda s: put(wbuf, owned_ref, wsem, s).wait())
    each(mats, lambda m: put(ubuf, update_ref, usem, m).wait())
    each(mats, lambda m: put(mbuf, mout_ref, msem, m).wait())


def per_device_planes(activations, cotangents, momentum, owners, bucket_starts):
    n_shard = lax.axis_size("shard")
    n_rep = lax.axis_size("rep")
    layers, tok_rows, width = activations.shape
    token_total = tok_rows * n_shard * n_rep
    cols = width // n_shard
    rows = KV // 2
    groups = n_rep // 2
    members = MATS // groups
    slots = -(-MATS // n_shard) + 1
    update_scale = math.sqrt(max(KV, D))
    bf16, f32, i32 = jnp.bfloat16, jnp.float32, jnp.int32
    z = lax.axis_index("shard")
    my_group = lax.axis_index("rep") // 2

    index = jnp.arange(MATS, dtype=i32)
    before = (owners[None, :] < owners[:, None]) | (
        (owners[None, :] == owners[:, None]) & (index[None, :] < index[:, None])
    )
    rank = jnp.sum(before.astype(i32), axis=1)
    position = (rank % groups) * members + rank // groups
    perm = jnp.sum(jnp.where(position[None, :] == index[:, None], index[None, :], 0), axis=1)
    start = jnp.sum((owners < z).astype(i32))
    count = jnp.sum((owners == z).astype(i32))

    params = functools.partial(
        pltpu.CompilerParams, has_side_effects=True, vmem_limit_bytes=VMEM_LIMIT
    )
    dma = pltpu.SemaphoreType.DMA
    gall, sq = pl.pallas_call(
        functools.partial(reduce_kernel, n_shard, 1.0 / math.sqrt(token_total)),
        out_shape=(
            jax.ShapeDtypeStruct((n_rep, members, rows, cols), bf16),
            jax.ShapeDtypeStruct((n_shard, n_rep, members, 1, cols), f32),
        ),
        in_specs=[SMEM_SPEC, SMEM_SPEC, ANY_SPEC, ANY_SPEC],
        out_specs=(VMEM_SPEC, VMEM_SPEC),
        scratch_shapes=[
            pltpu.VMEM((layers, 2 * tok_rows, width), bf16),
            pltpu.VMEM((layers, 2 * tok_rows, 2 * KV), bf16),
            pltpu.VMEM((n_shard, 2, 2, members, rows, cols), bf16),
            pltpu.VMEM((n_shard, 2, members, rows, cols), bf16),
            pltpu.VMEM((n_shard, members, rows, cols), bf16),
            pltpu.VMEM((n_shard, members, rows, cols), bf16),
            pltpu.VMEM((n_shard, members, rows, cols), bf16),
            pltpu.VMEM((n_shard - 1, members, rows, cols), bf16),
            dma((2,)), dma((2,)), dma((2,)),
            dma((n_shard,)), dma((n_shard,)), dma((n_shard,)), dma((n_shard,)),
            dma((n_shard,)), dma((n_shard,)),
            dma((10,)), dma((10,)), dma((n_shard - 1,)), dma((n_shard - 1,)),
        ],
        compiler_params=params(collective_id=0),
        name="reduce",
    )(perm // 2, perm % 2, activations, cotangents)

    by_position = jnp.sum(
        sq.reshape(n_shard, groups, 2, members, cols), axis=(0, 2, 4)
    ).reshape(MATS)
    square_sums = jnp.sum(
        jnp.where(position[:, None] == index[None, :], by_position[None, :], 0.0), axis=1
    )
    factors = clip_factors(square_sums, bucket_starts)

    planes = jnp.arange(n_shard, dtype=i32)
    firsts = jnp.sum((owners[None, :] < planes[:, None]).astype(i32), axis=1)
    ranks = jnp.minimum(firsts + (my_group - firsts) % groups, MATS - 1)
    places = ranks // groups
    at_place = my_group * members + places
    mats = jnp.sum(
        jnp.where(position[None, :] == at_place[:, None], index[None, :], 0), axis=1
    )
    full = pl.pallas_call(
        functools.partial(spread_kernel, n_shard),
        out_shape=jax.ShapeDtypeStruct((KV, width), bf16),
        in_specs=[SMEM_SPEC, SMEM_SPEC, SMEM_SPEC, VMEM_SPEC, VMEM_SPEC],
        out_specs=VMEM_SPEC,
        scratch_shapes=[pltpu.VMEM((n_shard - 1, rows, cols), bf16)]
        + [dma((n_shard - 1,)) for _ in range(4)],
        compiler_params=params(collective_id=1),
        name="spread",
    )(mats, places, factors, momentum, gall)

    result = pl.pallas_call(
        newton_kernel,
        out_shape=jax.ShapeDtypeStruct((KV, width), bf16),
        in_specs=[VMEM_SPEC],
        out_specs=VMEM_SPEC,
        name="newton",
    )(full)

    member = my_group * members + jnp.arange(members, dtype=i32)
    owner = jnp.sum(
        jnp.where(position[None, :] == member[:, None], owners[None, :], 0), axis=1
    )
    oall, whole = pl.pallas_call(
        functools.partial(share_kernel, n_shard),
        out_shape=(
            jax.ShapeDtypeStruct((n_rep, members, rows, cols), bf16),
            jax.ShapeDtypeStruct((n_rep, rows, width), bf16),
        ),
        in_specs=[SMEM_SPEC, VMEM_SPEC],
        out_specs=(VMEM_SPEC, VMEM_SPEC),
        scratch_shapes=[pltpu.VMEM((n_shard, rows, cols), bf16)]
        + [dma((n_shard - 1,)) for _ in range(2)]
        + [dma((10,)) for _ in range(4)],
        compiler_params=params(collective_id=2),
        name="share",
    )(owner, result)

    slot = jnp.arange(slots, dtype=i32)
    momentum_out, update, owned = pl.pallas_call(
        functools.partial(finish_kernel, update_scale),
        out_shape=(
            jax.ShapeDtypeStruct(momentum.shape, f32),
            jax.ShapeDtypeStruct(momentum.shape, f32),
            jax.ShapeDtypeStruct((slots, KV, width), bf16),
        ),
        in_specs=[SMEM_SPEC] * 5 + [VMEM_SPEC] * 3 + [ANY_SPEC],
        out_specs=(ANY_SPEC,) * 3,
        scratch_shapes=[
            pltpu.VMEM(momentum.shape, f32),
            pltpu.VMEM(momentum.shape, f32),
            pltpu.VMEM((slots, KV, width), bf16),
            dma((MATS,)), dma((MATS,)), dma((MATS,)), dma((slots,)),
        ],
        compiler_params=pltpu.CompilerParams(vmem_limit_bytes=VMEM_LIMIT),
        name="finish",
    )(
        2 * (position // members), position % members, factors,
        2 * ((start + slot) % groups), (slot < count).astype(f32),
        gall, oall, whole, momentum,
    )
    return (momentum_out, update, owned)


def solution(mesh):
    groups = mesh.shape["rep"] // 2
    slots = -(-MATS // mesh.shape["shard"]) + 1
    fits = mesh.shape["rep"] == 8 and MATS % groups == 0 and slots <= groups
    placed = (
        P(None, ("rep", "shard"), None),
        P(None, ("rep", "shard"), None),
        P(None, None, "shard"),
        P(),
        P(),
    )
    return jax.shard_map(
        per_device_planes if fits else per_device_general,
        mesh=mesh,
        in_specs=placed,
        out_specs=(P(None, None, "shard"), P(None, None, "shard"), P("shard", None, None)),
        check_vma=False,
    )
```

```python
import functools
import math

import jax
import jax.numpy as jnp
from jax import lax
from jax.experimental import pallas as pl
from jax.experimental.pallas import tpu as pltpu
from jax.sharding import PartitionSpec as P

D = 2048
KV = 256
ITERS = 5
MATS = 12
MESH = pl.DeviceIdType.MESH
VMEM_SPEC = pl.BlockSpec(memory_space=pltpu.VMEM)
SMEM_SPEC = pl.BlockSpec(memory_space=pltpu.SMEM)
ANY_SPEC = pl.BlockSpec(memory_space=pl.ANY)
VMEM_LIMIT = 60 * 1024 * 1024

coef_a = 3.4445
coef_b = -4.775
coef_c = 2.0315
momentum_rate = 0.95
clip_level = 0.5
epsilon = 1e-06


def orthogonal_batch(matrices):
    values = matrices.astype(jnp.float32)
    frobenius = jnp.sqrt(jnp.sum(values * values, axis=(1, 2), keepdims=True))
    matrix = (values / (frobenius + epsilon)).astype(jnp.bfloat16)
    for iteration in range(ITERS):
        gram_matrix = jnp.einsum(
            "skd,sjd->skj", matrix, matrix, preferred_element_type=jnp.float32
        ).astype(jnp.bfloat16)
        square = jnp.einsum(
            "skj,sji->ski", gram_matrix, gram_matrix, preferred_element_type=jnp.float32
        )
        mixing = (coef_b * gram_matrix.astype(jnp.float32) + coef_c * square).astype(jnp.bfloat16)
        product = jnp.einsum("skj,sjd->skd", mixing, matrix, preferred_element_type=jnp.float32)
        matrix = (coef_a * matrix.astype(jnp.float32) + product).astype(jnp.bfloat16)
    return matrix


def clip_factors(square_sums, bucket_starts):
    indices = jnp.arange(MATS, dtype=jnp.int32)
    buckets = jnp.sum((indices[:, None] >= bucket_starts[None, :]).astype(jnp.int32), axis=1)
    together = (buckets[:, None] == buckets[None, :]).astype(jnp.float32)
    totals = jnp.sum(together * square_sums[None, :], axis=1)
    members = jnp.sum(together, axis=1)
    root_mean = jnp.sqrt(totals / (members * KV * D) + epsilon)
    return jnp.minimum(1.0, clip_level / root_mean)


def slot_numbers(owners):
    indices = jnp.arange(MATS, dtype=jnp.int32)
    earlier = (indices[None, :] < indices[:, None]) & (owners[None, :] == owners[:, None])
    return jnp.sum(earlier.astype(jnp.int32), axis=1)


def selector(owner_of, slot_of, shard_count, slot_count):
    holders = lax.broadcasted_iota(jnp.int32, (shard_count, slot_count, 1), 0)
    places = lax.broadcasted_iota(jnp.int32, (shard_count, slot_count, 1), 1)
    chosen = (holders == owner_of[None, None, :]) & (places == slot_of[None, None, :])
    return chosen.astype(jnp.bfloat16)


def pack_slots(shards, chooser):
    return jnp.einsum("psm,mkd->skpd", chooser, shards, preferred_element_type=jnp.float32).astype(
        jnp.bfloat16
    )


def unpack_slots(received, chooser):
    return jnp.einsum("psm,skpd->mkd", chooser, received, preferred_element_type=jnp.float32)


def per_device_general(activations, cotangents, momentum, owners, bucket_starts):
    shard_count = lax.axis_size("shard")
    replica_count = lax.axis_size("rep")
    layers, tok_rows, width = activations.shape
    token_total = tok_rows * shard_count * replica_count
    columns = width // shard_count
    slot_count = -(-MATS // shard_count) + 1
    update_scale = math.sqrt(max(KV, D))
    partial_terms = jnp.einsum(
        "ltk,ltd->lkd", cotangents, activations, preferred_element_type=jnp.float32
    ).reshape(MATS, KV, width)
    shard_part = lax.psum_scatter(
        partial_terms.astype(jnp.bfloat16), "shard", scatter_dimension=2, tiled=True
    )
    summed = lax.psum(shard_part, "rep").astype(jnp.float32)
    gradient = summed / jnp.sqrt(jnp.float32(token_total))
    square_sums = lax.psum(jnp.sum(gradient * gradient, axis=(1, 2)), "shard")
    factors = clip_factors(square_sums, bucket_starts)
    momentum_out = momentum_rate * momentum + factors[:, None, None] * gradient
    nesterov = (factors[:, None, None] * gradient + momentum_rate * momentum_out).astype(
        jnp.bfloat16
    )
    slot_of = slot_numbers(owners)
    chooser = selector(owners, slot_of, shard_count, slot_count)
    received = lax.all_to_all(
        pack_slots(nesterov, chooser), "shard", split_axis=2, concat_axis=2, tiled=True
    )
    item_count = received.shape[0]
    result = orthogonal_batch(received.reshape(item_count, KV, width))
    scaled = (update_scale * result.astype(jnp.float32)).astype(jnp.bfloat16)
    returned_part = lax.all_to_all(
        result.reshape(item_count, KV, shard_count, columns),
        "shard",
        split_axis=2,
        concat_axis=2,
        tiled=True,
    )
    update = update_scale * unpack_slots(returned_part, chooser)
    return (momentum_out, update, scaled)


def place():
    me = lax.axis_index("rep")
    core = lax.rem(me, 2)
    x = lax.rem(lax.div(me, 2), 2)
    y = lax.div(me, 4)
    to_core = me + 1 - 2 * core
    to_x = me + 2 - 4 * x
    to_y = me + 4 - 8 * y
    to_xy = me + 6 - 4 * x - 8 * y
    return me, core, x, y, to_core, to_x, to_y, to_xy


def greet(peers):
    barrier = pltpu.get_barrier_semaphore()
    for peer in peers:
        pl.semaphore_signal(barrier, inc=1, device_id=peer, device_id_type=MESH)
    pl.semaphore_wait(barrier, len(peers))


def remote(src, dst, send, recv, peer):
    return pltpu.make_async_remote_copy(
        src_ref=src, dst_ref=dst, send_sem=send, recv_sem=recv, device_id=peer, device_id_type=MESH
    )


def plane_gather_start(z, at, send, recv):
    me, core, x, y, to_core, to_x, to_y, to_xy = place()
    plan = ((0, to_x, 0), (2, to_y, 1), (1, to_x, 1), (3, to_y, 0), (4, to_core, None))
    copies = {}
    for k, peer, half in plan:
        copies[k] = remote(at(me, half), at(me, half), send.at[k], recv.at[k], (peer, z))
        copies[k].start()
    return copies


def plane_gather_turn(z, at, send, recv, copies):
    me, core, x, y, to_core, to_x, to_y, to_xy = place()

    def forward(k, block, half, peer):
        copies[k] = remote(
            at(block, half), at(block, half), send.at[k], recv.at[k], (peer, z)
        )
        copies[k].start()

    copies[0].wait_recv()
    forward(5, to_x, 0, to_y)
    copies[2].wait_recv()
    forward(6, to_y, 1, to_x)
    copies[1].wait_recv()
    forward(7, to_x, None, to_core)
    copies[3].wait_recv()
    forward(8, to_y, None, to_core)


def plane_gather_finish(z, at, send, recv, copies):
    me, core, x, y, to_core, to_x, to_y, to_xy = place()
    copies[5].wait_recv()
    copies[6].wait_recv()
    copies[9] = remote(
        at(to_xy, None), at(to_xy, None), send.at[9], recv.at[9], (to_core, z)
    )
    copies[9].start()
    for k in (4, 7, 8, 9):
        copies[k].wait_recv()
    for k in range(10):
        copies[k].wait_send()


def block_at(ref, axis):
    rows = ref.shape[axis] // 2

    def at(r, half):
        if half is None:
            return ref.at[r]
        cut = pl.ds(half * rows, rows)
        return ref.at[r, cut] if axis == 1 else ref.at[r, :, cut]

    return at


def plan_kernel(
    n_shard, groups, owner_of, lay_ref, half_ref, position_ref, block_ref, member_ref,
    mat_ref, place_ref, owner_ref, slot_ref, keep_ref, perm, sort,
):
    z = lax.axis_index("shard")
    group = lax.div(lax.axis_index("rep"), 2)
    members = owner_ref.shape[0]
    owners = [owner_of[m] for m in range(MATS)]
    one = lambda yes: yes.astype(jnp.int32)
    for m in range(MATS):
        rank = jnp.int32(0)
        for j in range(MATS):
            if j != m:
                rank += one(owners[j] <= owners[m] if j < m else owners[j] < owners[m])
        member = lax.div(rank, groups)
        block = lax.rem(rank, groups)
        position = block * members + member
        position_ref[m] = position
        block_ref[m] = 2 * block
        member_ref[m] = member
        lay_ref[position] = jnp.int32(m // 2)
        half_ref[position] = jnp.int32(m % 2)
        perm[position] = jnp.int32(m)
        sort[position] = owners[m]
    for j in range(members):
        owner_ref[j] = sort[group * members + j]
    for p in range(n_shard):
        first = jnp.int32(0)
        for m in range(MATS):
            first += one(owners[m] < p)
        skip = lax.rem(group + groups * MATS - first, groups)
        place = lax.div(jnp.minimum(first + skip, MATS - 1), groups)
        place_ref[p] = place
        mat_ref[p] = perm[group * members + place]
    start = jnp.int32(0)
    count = jnp.int32(0)
    for m in range(MATS):
        start += one(owners[m] < z)
        count += one(owners[m] == z)
    for i in range(slot_ref.shape[0]):
        slot_ref[i] = 2 * lax.rem(start + i, groups)
        keep_ref[i] = one(count > i)


def reduce_kernel(
    n_shard, inverse, lay_ref, half_ref, act_ref, cot_ref, gown_ref, sq_ref,
    act, cot, part, recv1, turn, recv2, plane, zrecv,
    local_sem, in_send, in_recv, s1, r1, s2, r2, s3, r3, gs, gr, qs, qr,
):
    me, core, x, y, to_core, to_x, to_y, to_xy = place()
    z = lax.axis_index("shard")
    tokens = act_ref.shape[1]
    rows, cols = part.shape[-2:]
    members = part.shape[2 + 1]
    steps = [d for d in (2, 1, 3) if d < n_shard] + list(range(4, n_shard)) + [0]
    other = 1 - 2 * core
    near = (to_core, to_x, to_y, to_xy, to_x + other, to_y + other, to_xy + other)
    peers = [(p, z) for p in near]
    peers += [(me, lax.rem(z + d, n_shard)) for d in range(1, n_shard)]
    own = [
        pltpu.make_async_copy(act_ref, act.at[:, pl.ds(0, tokens)], local_sem.at[0]),
        pltpu.make_async_copy(cot_ref, cot.at[:, pl.ds(0, tokens)], local_sem.at[1]),
    ]
    for c in own:
        c.start()
    greet(peers)
    swap = [
        remote(cot_ref, cot.at[:, pl.ds(tokens, tokens)], in_send.at[1], in_recv.at[1], (to_core, z)),
        remote(act_ref, act.at[:, pl.ds(tokens, tokens)], in_send.at[0], in_recv.at[0], (to_core, z)),
    ]
    for c in swap:
        c.start()
    for c in own:
        c.wait()
    for c in swap:
        c.wait()
    first = []
    second = []
    third = []

    def launch(k):
        offset = pl.multiple_of(lax.rem(z + steps[k], n_shard) * cols, cols)

        def one(q, carry):
            group = lax.div(q, members)
            member = lax.rem(q, members)
            block = cot[lay_ref[q]]
            low = jnp.where(core == 0, block[:, :rows], block[:, rows : 2 * rows])
            high = jnp.where(core == 0, block[:, 2 * rows : 3 * rows], block[:, 3 * rows :])
            left = jnp.where(half_ref[q] == 0, low, high)
            right = act[lay_ref[q], :, pl.ds(offset, cols)]
            value = lax.dot_general(
                left, right, (((0,), (0,)), ((), ())), preferred_element_type=jnp.float32
            )
            part[k, lax.div(group, 2), lax.rem(group, 2), member] = value.astype(part.dtype)
            return carry

        lax.fori_loop(0, 4 * members, one, 0)

    def send_first(k):
        if k % 2 == 0:
            c = remote(part.at[k, :, 1 - x], recv1.at[k], s1.at[k], r1.at[k], (to_x, z))
        else:
            c = remote(part.at[k, 1 - y], recv1.at[k], s1.at[k], r1.at[k], (to_y, z))
        c.start()
        first.append(c)

    def send_second(k):
        first[k].wait_recv()

        def add_out(j, carry):
            if k % 2 == 0:
                mine = part[k, 1 - y, x, j]
                came = recv1[k, 1 - y, j]
            else:
                mine = part[k, y, 1 - x, j]
                came = recv1[k, 1 - x, j]
            turn[k, j] = (mine.astype(jnp.float32) + came.astype(jnp.float32)).astype(turn.dtype)
            return carry

        lax.fori_loop(0, members, add_out, 0)
        c = remote(
            turn.at[k], recv2.at[k], s2.at[k], r2.at[k], (to_y if k % 2 == 0 else to_x, z)
        )
        c.start()
        second.append(c)

    def send_third(k):
        second[k].wait_recv()

        def add_in(j, carry):
            came = recv1[k, y, j] if k % 2 == 0 else recv1[k, x, j]
            value = part[k, y, x, j].astype(jnp.float32) + came.astype(jnp.float32)
            value = value + recv2[k, j].astype(jnp.float32)
            plane[k, j] = value.astype(plane.dtype)
            return carry

        lax.fori_loop(0, members, add_in, 0)
        if steps[k]:
            c = remote(
                plane.at[k], zrecv.at[k], s3.at[k], r3.at[k],
                (me, lax.rem(z + steps[k], n_shard)),
            )
            c.start()
            third.append(c)

    launch(0)
    send_first(0)
    launch(1)
    send_first(1)
    for k in range(2, n_shard):
        launch(k)
    for k in range(0, n_shard, 2):
        pair = [i for i in (k, k + 1) if i < n_shard]
        for i in pair:
            send_second(i)
        for i in (k + 2, k + 3):
            if i < n_shard:
                send_first(i)
        for i in pair:
            send_third(i)
    for c in third:
        c.wait_recv()

    def add_last(j, carry):
        value = plane[n_shard - 1, j].astype(jnp.float32)
        for k in range(n_shard - 1):
            value = value + zrecv[k, j].astype(jnp.float32)
        value = (value * inverse).astype(gown_ref.dtype)
        gown_ref[core, j] = value
        value = value.astype(jnp.float32)
        line = jnp.sum(value * value, axis=0, keepdims=True)
        lanes = sq_ref.shape[-1]
        fold = line[:, :lanes]
        for i in range(1, cols // lanes):
            fold = fold + line[:, i * lanes : (i + 1) * lanes]
        sq_ref[0, me, j] = fold
        return carry

    lax.fori_loop(0, members, add_last, 0)
    fourth = []
    for k, peer in enumerate(near):
        c = remote(sq_ref.at[0, me], sq_ref.at[0, me], gs.at[k], gr.at[k], (peer, z))
        c.start()
        fourth.append(c)
    c = remote(gown_ref.at[core], gown_ref.at[core], gs.at[len(near)], gr.at[len(near)], (to_core, z))
    c.start()
    for f in fourth:
        f.wait_recv()
    for d in range(1, n_shard):
        f = remote(
            sq_ref.at[0], sq_ref.at[d], qs.at[d - 1], qr.at[d - 1],
            (me, lax.rem(z + d, n_shard)),
        )
        f.start()
        fourth.append(f)
    for f in fourth[len(near):]:
        f.wait_recv()
    c.wait_recv()
    for f in fourth + [c]:
        f.wait_send()
    for c in first + second + third:
        c.wait_send()


def spread_kernel(
    n_shard, mat_ref, place_ref, factor_ref, momentum_ref, gown_ref, full_ref, gall_ref,
    held, zs, zr, cs, cr, gs, gr,
):
    me, core, x, y, to_core, to_x, to_y, to_xy = place()
    z = lax.axis_index("shard")
    rows = full_ref.shape[0] // 2
    cols = full_ref.shape[1] // n_shard

    def at(side, shard):
        return (
            pl.ds(pl.multiple_of(side * rows, rows), rows),
            pl.ds(pl.multiple_of(shard * cols, cols), cols),
        )

    def nesterov(p, side):
        matrix = mat_ref[p]
        half = pl.ds(pl.multiple_of(side * rows, rows), rows)
        step = factor_ref[matrix] * gown_ref[side, place_ref[p]].astype(jnp.float32)
        new = momentum_rate * momentum_ref[matrix, half] + step
        return (step + momentum_rate * new).astype(full_ref.dtype)

    order = [d for d in (2, 1, 3) if d < n_shard] + list(range(4, n_shard))
    for d in order:
        held[d - 1] = nesterov(lax.rem(z + d, n_shard), core)
    gall_ref[me] = gown_ref[core]
    greet(
        [(p, z) for p in (to_core, to_x, to_y)]
        + [(me, lax.rem(z + d, n_shard)) for d in range(1, n_shard)]
    )
    copies = []
    for d in order:
        peer = (me, lax.rem(z + d, n_shard))
        c = remote(held.at[d - 1], full_ref.at[at(core, z)], zs.at[d - 1], zr.at[d - 1], peer)
        c.start()
        copies.append(c)
    at_g = block_at(gall_ref, 2)
    gathers = plane_gather_start(z, at_g, gs, gr)
    for side in range(2):
        full_ref[at(side, z)] = nesterov(z, side)
    onward = []
    for c, d in zip(copies, order):
        c.wait_recv()
        source = full_ref.at[at(core, lax.rem(z + n_shard - d, n_shard))]
        f = remote(source, source, cs.at[d - 1], cr.at[d - 1], (to_core, z))
        f.start()
        onward.append(f)
        if len(onward) == 1:
            plane_gather_turn(z, at_g, gs, gr, gathers)
    for f in onward:
        f.wait_recv()
    plane_gather_finish(z, at_g, gs, gr, gathers)
    for c in copies + onward:
        c.wait_send()


def newton_kernel(u_ref, o_ref):
    def total(i, carry):
        value = u_ref[pl.ds(pl.multiple_of(i * 32, 32), 32), :].astype(jnp.float32)
        return carry + jnp.sum(value * value, axis=0, keepdims=True)

    kv, width = u_ref.shape
    sums = lax.fori_loop(0, kv // 32, total, jnp.zeros((1, width), jnp.float32))
    inverse = 1.0 / (jnp.sqrt(jnp.sum(sums, axis=1, keepdims=True)) + epsilon)
    matrix = (u_ref[...].astype(jnp.float32) * inverse).astype(jnp.bfloat16)
    for iteration in range(ITERS):
        gram = lax.dot_general(
            matrix, matrix, (((1,), (1,)), ((), ())), preferred_element_type=jnp.float32
        ).astype(jnp.bfloat16)
        square = jnp.dot(gram, gram, preferred_element_type=jnp.float32)
        mixing = (coef_b * gram.astype(jnp.float32) + coef_c * square).astype(jnp.bfloat16)
        product = jnp.dot(mixing, matrix, preferred_element_type=jnp.float32)
        matrix = (coef_a * matrix.astype(jnp.float32) + product).astype(jnp.bfloat16)
    o_ref[...] = matrix


def share_kernel(
    n_shard, owner_ref, o_ref, oall_ref, whole_ref, back, bs, br, us, ur, ws, wr
):
    me, core, x, y, to_core, to_x, to_y, to_xy = place()
    z = lax.axis_index("shard")
    rows = o_ref.shape[0] // 2
    cols = o_ref.shape[1] // n_shard
    half = pl.ds(pl.multiple_of(core * rows, rows), rows)

    def piece(shard):
        return half, pl.ds(pl.multiple_of(shard * cols, cols), cols)

    peers = [(p, z) for p in (to_core, to_x, to_y)]
    peers += [(me, lax.rem(z + d, n_shard)) for d in range(1, n_shard)]
    greet(peers)
    order = [d for d in (2, 1, 3) if d < n_shard] + list(range(4, n_shard))
    returns = []
    for d in order:
        to = lax.rem(z + d, n_shard)
        c = remote(o_ref.at[piece(to)], back.at[z], bs.at[d - 1], br.at[d - 1], (me, to))
        c.start()
        returns.append(c)
    whole_ref[me] = o_ref[half]
    at_w = block_at(whole_ref, 1)
    at_u = block_at(oall_ref, 2)
    cw = plane_gather_start(z, at_w, ws, wr)
    back[z] = o_ref[piece(z)]
    for c in returns:
        c.wait_recv()
    for j in range(oall_ref.shape[1]):
        oall_ref[me, j] = back[owner_ref[j]]
    cu = plane_gather_start(z, at_u, us, ur)
    plane_gather_turn(z, at_w, ws, wr, cw)
    plane_gather_turn(z, at_u, us, ur, cu)
    plane_gather_finish(z, at_w, ws, wr, cw)
    plane_gather_finish(z, at_u, us, ur, cu)
    for c in returns:
        c.wait_send()


def finish_kernel(
    scale, block_ref, member_ref, factor_ref, slot_ref, keep_ref,
    gall_ref, oall_ref, whole_ref, momentum_ref, mout_ref, update_ref, owned_ref,
    mbuf, ubuf, wbuf, load, msem, usem, wsem,
):
    mats = mbuf.shape[0]
    slots = wbuf.shape[0]
    rows = gall_ref.shape[2]

    def fetch(m):
        return pltpu.make_async_copy(momentum_ref.at[m], mbuf.at[m], load.at[m])

    def put(buf, out, sem, m):
        return pltpu.make_async_copy(buf.at[m], out.at[m], sem.at[m])

    def each(count, body):
        def step(m, carry):
            body(m)
            return carry

        lax.fori_loop(0, count, step, 0)

    each(mats, lambda m: fetch(m).start())

    def owned_one(s):
        for c in range(2):
            value = scale * whole_ref[slot_ref[s] + c].astype(jnp.float32)
            wbuf[s, pl.ds(c * rows, rows)] = (value * keep_ref[s].astype(jnp.float32)).astype(wbuf.dtype)
        put(wbuf, owned_ref, wsem, s).start()

    def update_one(m):
        for c in range(2):
            value = oall_ref[block_ref[m] + c, member_ref[m]].astype(jnp.float32)
            ubuf[m, pl.ds(c * rows, rows)] = scale * value
        put(ubuf, update_ref, usem, m).start()

    def momentum_one(m):
        fetch(m).wait()
        for c in range(2):
            cut = pl.ds(c * rows, rows)
            step = factor_ref[m] * gall_ref[block_ref[m] + c, member_ref[m]].astype(jnp.float32)
            mbuf[m, cut] = momentum_rate * mbuf[m, cut] + step
        put(mbuf, mout_ref, msem, m).start()

    each(slots, owned_one)
    each(mats, update_one)
    each(mats, momentum_one)
    each(slots, lambda s: put(wbuf, owned_ref, wsem, s).wait())
    each(mats, lambda m: put(ubuf, update_ref, usem, m).wait())
    each(mats, lambda m: put(mbuf, mout_ref, msem, m).wait())


def per_device_planes(activations, cotangents, momentum, owners, bucket_starts):
    n_shard = lax.axis_size("shard")
    n_rep = lax.axis_size("rep")
    layers, tok_rows, width = activations.shape
    token_total = tok_rows * n_shard * n_rep
    cols = width // n_shard
    rows = KV // 2
    lanes = math.gcd(cols, 128)
    groups = n_rep // 2
    members = MATS // groups
    slots = -(-MATS // n_shard) + 1
    update_scale = math.sqrt(max(KV, D))
    bf16, f32, i32 = jnp.bfloat16, jnp.float32, jnp.int32
    shapes = [MATS] * 5 + [n_shard] * 2 + [members] + [slots] * 2
    lay, half, position, block, member, mats, places, owner, slot_block, slot_keep = pl.pallas_call(
        functools.partial(plan_kernel, n_shard, groups),
        out_shape=[jax.ShapeDtypeStruct((n,), i32) for n in shapes],
        in_specs=[SMEM_SPEC],
        out_specs=[SMEM_SPEC] * len(shapes),
        scratch_shapes=[pltpu.SMEM((MATS,), i32), pltpu.SMEM((MATS,), i32)],
        name="plan",
    )(owners)
    index = jnp.arange(MATS, dtype=i32)

    params = functools.partial(
        pltpu.CompilerParams, has_side_effects=True, vmem_limit_bytes=VMEM_LIMIT
    )
    dma = pltpu.SemaphoreType.DMA
    gown, sq = pl.pallas_call(
        functools.partial(reduce_kernel, n_shard, 1.0 / math.sqrt(token_total)),
        out_shape=(
            jax.ShapeDtypeStruct((2, members, rows, cols), bf16),
            jax.ShapeDtypeStruct((n_shard, n_rep, members, 1, lanes), f32),
        ),
        in_specs=[SMEM_SPEC, SMEM_SPEC, ANY_SPEC, ANY_SPEC],
        out_specs=(VMEM_SPEC, VMEM_SPEC),
        scratch_shapes=[
            pltpu.VMEM((layers, 2 * tok_rows, width), bf16),
            pltpu.VMEM((layers, 2 * tok_rows, 2 * KV), bf16),
            pltpu.VMEM((n_shard, 2, 2, members, rows, cols), bf16),
            pltpu.VMEM((n_shard, 2, members, rows, cols), bf16),
            pltpu.VMEM((n_shard, members, rows, cols), bf16),
            pltpu.VMEM((n_shard, members, rows, cols), bf16),
            pltpu.VMEM((n_shard, members, rows, cols), bf16),
            pltpu.VMEM((n_shard - 1, members, rows, cols), bf16),
            dma((2,)), dma((2,)), dma((2,)),
            dma((n_shard,)), dma((n_shard,)), dma((n_shard,)), dma((n_shard,)),
            dma((n_shard,)), dma((n_shard,)),
            dma((8,)), dma((8,)), dma((n_shard - 1,)), dma((n_shard - 1,)),
        ],
        compiler_params=params(collective_id=0),
        name="reduce",
    )(lay, half, activations, cotangents)

    by_position = jnp.sum(
        sq.reshape(n_shard, groups, 2, members, lanes), axis=(0, 2, 4)
    ).reshape(MATS)
    square_sums = jnp.sum(
        jnp.where(position[:, None] == index[None, :], by_position[None, :], 0.0), axis=1
    )
    factors = clip_factors(square_sums, bucket_starts)

    full, gall = pl.pallas_call(
        functools.partial(spread_kernel, n_shard),
        out_shape=(
            jax.ShapeDtypeStruct((KV, width), bf16),
            jax.ShapeDtypeStruct((n_rep, members, rows, cols), bf16),
        ),
        in_specs=[SMEM_SPEC, SMEM_SPEC, SMEM_SPEC, VMEM_SPEC, VMEM_SPEC],
        out_specs=(VMEM_SPEC, VMEM_SPEC),
        scratch_shapes=[pltpu.VMEM((n_shard - 1, rows, cols), bf16)]
        + [dma((n_shard - 1,)) for _ in range(4)]
        + [dma((10,)) for _ in range(2)],
        compiler_params=params(collective_id=1),
        name="spread",
    )(mats, places, factors, momentum, gown)

    result = pl.pallas_call(
        newton_kernel,
        out_shape=jax.ShapeDtypeStruct((KV, width), bf16),
        in_specs=[VMEM_SPEC],
        out_specs=VMEM_SPEC,
        name="newton",
    )(full)

    oall, whole = pl.pallas_call(
        functools.partial(share_kernel, n_shard),
        out_shape=(
            jax.ShapeDtypeStruct((n_rep, members, rows, cols), bf16),
            jax.ShapeDtypeStruct((n_rep, rows, width), bf16),
        ),
        in_specs=[SMEM_SPEC, VMEM_SPEC],
        out_specs=(VMEM_SPEC, VMEM_SPEC),
        scratch_shapes=[pltpu.VMEM((n_shard, rows, cols), bf16)]
        + [dma((n_shard - 1,)) for _ in range(2)]
        + [dma((10,)) for _ in range(4)],
        compiler_params=params(collective_id=2),
        name="share",
    )(owner, result)

    momentum_out, update, owned = pl.pallas_call(
        functools.partial(finish_kernel, update_scale),
        out_shape=(
            jax.ShapeDtypeStruct(momentum.shape, f32),
            jax.ShapeDtypeStruct(momentum.shape, f32),
            jax.ShapeDtypeStruct((slots, KV, width), bf16),
        ),
        in_specs=[SMEM_SPEC] * 5 + [VMEM_SPEC] * 3 + [ANY_SPEC],
        out_specs=(ANY_SPEC,) * 3,
        scratch_shapes=[
            pltpu.VMEM(momentum.shape, f32),
            pltpu.VMEM(momentum.shape, f32),
            pltpu.VMEM((slots, KV, width), bf16),
            dma((MATS,)), dma((MATS,)), dma((MATS,)), dma((slots,)),
        ],
        compiler_params=pltpu.CompilerParams(vmem_limit_bytes=VMEM_LIMIT),
        name="finish",
    )(
        block, member, factors, slot_block, slot_keep,
        gall, oall, whole, momentum,
    )
    return (momentum_out, update, owned)


def solution(mesh):
    groups = mesh.shape["rep"] // 2
    slots = -(-MATS // mesh.shape["shard"]) + 1
    fits = mesh.shape["rep"] == 8 and MATS % groups == 0 and slots <= groups
    placed = (
        P(None, ("rep", "shard"), None),
        P(None, ("rep", "shard"), None),
        P(None, None, "shard"),
        P(),
        P(),
    )
    return jax.shard_map(
        per_device_planes if fits else per_device_general,
        mesh=mesh,
        in_specs=placed,
        out_specs=(P(None, None, "shard"), P(None, None, "shard"), P("shard", None, None)),
        check_vma=False,
    )
```

```python
import functools
import math

import jax
import jax.numpy as jnp
from jax import lax
from jax.experimental import pallas as pl
from jax.experimental.pallas import tpu as pltpu
from jax.sharding import PartitionSpec as P

D = 2048
KV = 256
ITERS = 5
MATS = 12
MESH = pl.DeviceIdType.MESH
VMEM_SPEC = pl.BlockSpec(memory_space=pltpu.VMEM)
SMEM_SPEC = pl.BlockSpec(memory_space=pltpu.SMEM)
ANY_SPEC = pl.BlockSpec(memory_space=pl.ANY)
VMEM_LIMIT = 60 * 1024 * 1024

coef_a = 3.4445
coef_b = -4.775
coef_c = 2.0315
momentum_rate = 0.95
clip_level = 0.5
epsilon = 1e-06


def orthogonal_batch(matrices):
    values = matrices.astype(jnp.float32)
    frobenius = jnp.sqrt(jnp.sum(values * values, axis=(1, 2), keepdims=True))
    matrix = (values / (frobenius + epsilon)).astype(jnp.bfloat16)
    for iteration in range(ITERS):
        gram_matrix = jnp.einsum(
            "skd,sjd->skj", matrix, matrix, preferred_element_type=jnp.float32
        ).astype(jnp.bfloat16)
        square = jnp.einsum(
            "skj,sji->ski", gram_matrix, gram_matrix, preferred_element_type=jnp.float32
        )
        mixing = (coef_b * gram_matrix.astype(jnp.float32) + coef_c * square).astype(jnp.bfloat16)
        product = jnp.einsum("skj,sjd->skd", mixing, matrix, preferred_element_type=jnp.float32)
        matrix = (coef_a * matrix.astype(jnp.float32) + product).astype(jnp.bfloat16)
    return matrix


def clip_factors(square_sums, bucket_starts):
    indices = jnp.arange(MATS, dtype=jnp.int32)
    buckets = jnp.sum((indices[:, None] >= bucket_starts[None, :]).astype(jnp.int32), axis=1)
    together = (buckets[:, None] == buckets[None, :]).astype(jnp.float32)
    totals = jnp.sum(together * square_sums[None, :], axis=1)
    members = jnp.sum(together, axis=1)
    root_mean = jnp.sqrt(totals / (members * KV * D) + epsilon)
    return jnp.minimum(1.0, clip_level / root_mean)


def slot_numbers(owners):
    indices = jnp.arange(MATS, dtype=jnp.int32)
    earlier = (indices[None, :] < indices[:, None]) & (owners[None, :] == owners[:, None])
    return jnp.sum(earlier.astype(jnp.int32), axis=1)


def selector(owner_of, slot_of, shard_count, slot_count):
    holders = lax.broadcasted_iota(jnp.int32, (shard_count, slot_count, 1), 0)
    places = lax.broadcasted_iota(jnp.int32, (shard_count, slot_count, 1), 1)
    chosen = (holders == owner_of[None, None, :]) & (places == slot_of[None, None, :])
    return chosen.astype(jnp.bfloat16)


def pack_slots(shards, chooser):
    return jnp.einsum("psm,mkd->skpd", chooser, shards, preferred_element_type=jnp.float32).astype(
        jnp.bfloat16
    )


def unpack_slots(received, chooser):
    return jnp.einsum("psm,skpd->mkd", chooser, received, preferred_element_type=jnp.float32)


def per_device_general(activations, cotangents, momentum, owners, bucket_starts):
    shard_count = lax.axis_size("shard")
    replica_count = lax.axis_size("rep")
    layers, tok_rows, width = activations.shape
    token_total = tok_rows * shard_count * replica_count
    columns = width // shard_count
    slot_count = -(-MATS // shard_count) + 1
    update_scale = math.sqrt(max(KV, D))
    partial_terms = jnp.einsum(
        "ltk,ltd->lkd", cotangents, activations, preferred_element_type=jnp.float32
    ).reshape(MATS, KV, width)
    shard_part = lax.psum_scatter(
        partial_terms.astype(jnp.bfloat16), "shard", scatter_dimension=2, tiled=True
    )
    summed = lax.psum(shard_part, "rep").astype(jnp.float32)
    gradient = summed / jnp.sqrt(jnp.float32(token_total))
    square_sums = lax.psum(jnp.sum(gradient * gradient, axis=(1, 2)), "shard")
    factors = clip_factors(square_sums, bucket_starts)
    momentum_out = momentum_rate * momentum + factors[:, None, None] * gradient
    nesterov = (factors[:, None, None] * gradient + momentum_rate * momentum_out).astype(
        jnp.bfloat16
    )
    slot_of = slot_numbers(owners)
    chooser = selector(owners, slot_of, shard_count, slot_count)
    received = lax.all_to_all(
        pack_slots(nesterov, chooser), "shard", split_axis=2, concat_axis=2, tiled=True
    )
    item_count = received.shape[0]
    result = orthogonal_batch(received.reshape(item_count, KV, width))
    scaled = (update_scale * result.astype(jnp.float32)).astype(jnp.bfloat16)
    returned_part = lax.all_to_all(
        result.reshape(item_count, KV, shard_count, columns),
        "shard",
        split_axis=2,
        concat_axis=2,
        tiled=True,
    )
    update = update_scale * unpack_slots(returned_part, chooser)
    return (momentum_out, update, scaled)


def place():
    me = lax.axis_index("rep")
    core = lax.rem(me, 2)
    x = lax.rem(lax.div(me, 2), 2)
    y = lax.div(me, 4)
    to_core = me + 1 - 2 * core
    to_x = me + 2 - 4 * x
    to_y = me + 4 - 8 * y
    to_xy = me + 6 - 4 * x - 8 * y
    return me, core, x, y, to_core, to_x, to_y, to_xy


def greet(peers):
    barrier = pltpu.get_barrier_semaphore()
    for peer in peers:
        pl.semaphore_signal(barrier, inc=1, device_id=peer, device_id_type=MESH)
    pl.semaphore_wait(barrier, len(peers))


def remote(src, dst, send, recv, peer):
    return pltpu.make_async_remote_copy(
        src_ref=src, dst_ref=dst, send_sem=send, recv_sem=recv, device_id=peer, device_id_type=MESH
    )


def plane_gather_start(z, at, send, recv):
    me, core, x, y, to_core, to_x, to_y, to_xy = place()
    plan = ((0, to_x, 0), (2, to_y, 1), (1, to_x, 1), (3, to_y, 0), (4, to_core, None))
    copies = {}
    for k, peer, half in plan:
        copies[k] = remote(at(me, half), at(me, half), send.at[k], recv.at[k], (peer, z))
        copies[k].start()
    return copies


def plane_gather_turn(z, at, send, recv, copies):
    me, core, x, y, to_core, to_x, to_y, to_xy = place()

    def forward(k, block, half, peer):
        copies[k] = remote(
            at(block, half), at(block, half), send.at[k], recv.at[k], (peer, z)
        )
        copies[k].start()

    copies[0].wait_recv()
    forward(5, to_x, 0, to_y)
    copies[2].wait_recv()
    forward(6, to_y, 1, to_x)
    copies[1].wait_recv()
    forward(7, to_x, None, to_core)
    copies[3].wait_recv()
    forward(8, to_y, None, to_core)


def plane_gather_finish(z, at, send, recv, copies):
    me, core, x, y, to_core, to_x, to_y, to_xy = place()
    copies[5].wait_recv()
    copies[6].wait_recv()
    copies[9] = remote(
        at(to_xy, None), at(to_xy, None), send.at[9], recv.at[9], (to_core, z)
    )
    copies[9].start()
    for k in (4, 7, 8, 9):
        copies[k].wait_recv()
    for k in range(10):
        copies[k].wait_send()


def block_at(ref, axis):
    rows = ref.shape[axis] // 2

    def at(r, half):
        if half is None:
            return ref.at[r]
        cut = pl.ds(half * rows, rows)
        return ref.at[r, cut] if axis == 1 else ref.at[r, :, cut]

    return at


def plan_kernel(
    n_shard, groups, owner_of, lay_ref, half_ref, position_ref, block_ref, member_ref,
    mat_ref, place_ref, owner_ref, slot_ref, keep_ref, perm, sort,
):
    z = lax.axis_index("shard")
    group = lax.div(lax.axis_index("rep"), 2)
    members = owner_ref.shape[0]
    owners = [owner_of[m] for m in range(MATS)]
    one = lambda yes: yes.astype(jnp.int32)
    for m in range(MATS):
        rank = jnp.int32(0)
        for j in range(MATS):
            if j != m:
                rank += one(owners[j] <= owners[m] if j < m else owners[j] < owners[m])
        member = lax.div(rank, groups)
        block = lax.rem(rank, groups)
        position = block * members + member
        position_ref[m] = position
        block_ref[m] = 2 * block
        member_ref[m] = member
        lay_ref[position] = jnp.int32(m // 2)
        half_ref[position] = jnp.int32(m % 2)
        perm[position] = jnp.int32(m)
        sort[position] = owners[m]
    for j in range(members):
        owner_ref[j] = sort[group * members + j]
    for p in range(n_shard):
        first = jnp.int32(0)
        for m in range(MATS):
            first += one(owners[m] < p)
        skip = lax.rem(group + groups * MATS - first, groups)
        place = lax.div(jnp.minimum(first + skip, MATS - 1), groups)
        place_ref[p] = place
        mat_ref[p] = perm[group * members + place]
    start = jnp.int32(0)
    count = jnp.int32(0)
    for m in range(MATS):
        start += one(owners[m] < z)
        count += one(owners[m] == z)
    for i in range(slot_ref.shape[0]):
        slot_ref[i] = 2 * lax.rem(start + i, groups)
        keep_ref[i] = one(count > i)


def reduce_kernel(
    n_shard, inverse, lay_ref, half_ref, act_ref, cot_ref, gown_ref, sq_ref,
    act, cot, part, recv1, turn, recv2, plane, zrecv,
    local_sem, in_send, in_recv, s1, r1, s2, r2, s3, r3, gs, gr, qs, qr,
):
    me, core, x, y, to_core, to_x, to_y, to_xy = place()
    z = lax.axis_index("shard")
    tokens = act_ref.shape[1]
    rows, cols = part.shape[-2:]
    members = part.shape[2 + 1]
    steps = [d for d in (2, 1, 3) if d < n_shard] + list(range(4, n_shard)) + [0]
    other = 1 - 2 * core
    near = (to_core, to_x, to_y, to_xy, to_x + other, to_y + other, to_xy + other)
    peers = [(p, z) for p in near]
    peers += [(me, lax.rem(z + d, n_shard)) for d in range(1, n_shard)]
    cut = [
        pl.ds(pl.multiple_of(lax.rem(z + d, n_shard) * cols, cols), cols) for d in steps
    ]
    own = [
        pltpu.make_async_copy(
            act_ref.at[:, :, cut[k]], act[k].at[:, pl.ds(0, tokens)], local_sem.at[k]
        )
        for k in range(n_shard)
    ]
    own.append(
        pltpu.make_async_copy(cot_ref, cot.at[:, pl.ds(0, tokens)], local_sem.at[n_shard])
    )
    for c in own:
        c.start()
    greet(peers)
    theirs = pl.ds(tokens, tokens)
    swap = [
        remote(
            act_ref.at[:, :, cut[k]], act[k].at[:, theirs],
            in_send.at[k], in_recv.at[k], (to_core, z),
        )
        for k in range(n_shard)
    ]
    swap.append(
        remote(cot_ref, cot.at[:, theirs], in_send.at[n_shard], in_recv.at[n_shard], (to_core, z))
    )
    for c in swap[-1:] + swap[:-1]:
        c.start()
    for c in own:
        c.wait()
    swap[n_shard].wait()
    first = []
    second = []
    third = []

    def launch(k):
        swap[k].wait()

        def one(q, carry):
            group = lax.div(q, members)
            member = lax.rem(q, members)
            block = cot[lay_ref[q]]
            low = jnp.where(core == 0, block[:, :rows], block[:, rows : 2 * rows])
            high = jnp.where(core == 0, block[:, 2 * rows : 3 * rows], block[:, 3 * rows :])
            left = jnp.where(half_ref[q] == 0, low, high)
            right = act[k][lay_ref[q]]
            value = lax.dot_general(
                left, right, (((0,), (0,)), ((), ())), preferred_element_type=jnp.float32
            )
            part[k, lax.div(group, 2), lax.rem(group, 2), member] = value.astype(part.dtype)
            return carry

        lax.fori_loop(0, 4 * members, one, 0)

    def send_first(k):
        if k % 2 == 0:
            c = remote(part.at[k, :, 1 - x], recv1.at[k], s1.at[k], r1.at[k], (to_x, z))
        else:
            c = remote(part.at[k, 1 - y], recv1.at[k], s1.at[k], r1.at[k], (to_y, z))
        c.start()
        first.append(c)

    def send_second(k):
        first[k].wait_recv()

        def add_out(j, carry):
            if k % 2 == 0:
                mine = part[k, 1 - y, x, j]
                came = recv1[k, 1 - y, j]
            else:
                mine = part[k, y, 1 - x, j]
                came = recv1[k, 1 - x, j]
            turn[k, j] = (mine.astype(jnp.float32) + came.astype(jnp.float32)).astype(turn.dtype)
            return carry

        lax.fori_loop(0, members, add_out, 0)
        c = remote(
            turn.at[k], recv2.at[k], s2.at[k], r2.at[k], (to_y if k % 2 == 0 else to_x, z)
        )
        c.start()
        second.append(c)

    def send_third(k):
        second[k].wait_recv()

        def add_in(j, carry):
            came = recv1[k, y, j] if k % 2 == 0 else recv1[k, x, j]
            value = part[k, y, x, j].astype(jnp.float32) + came.astype(jnp.float32)
            value = value + recv2[k, j].astype(jnp.float32)
            plane[k, j] = value.astype(plane.dtype)
            return carry

        lax.fori_loop(0, members, add_in, 0)
        if steps[k]:
            c = remote(
                plane.at[k], zrecv.at[k], s3.at[k], r3.at[k],
                (me, lax.rem(z + steps[k], n_shard)),
            )
            c.start()
            third.append(c)

    launch(0)
    send_first(0)
    launch(1)
    send_first(1)
    for k in range(2, n_shard):
        launch(k)
    for k in range(0, n_shard, 2):
        pair = [i for i in (k, k + 1) if i < n_shard]
        for i in pair:
            send_second(i)
        for i in (k + 2, k + 3):
            if i < n_shard:
                send_first(i)
        for i in pair:
            send_third(i)
    for c in third:
        c.wait_recv()

    def add_last(j, carry):
        value = plane[n_shard - 1, j].astype(jnp.float32)
        for k in range(n_shard - 1):
            value = value + zrecv[k, j].astype(jnp.float32)
        value = (value * inverse).astype(gown_ref.dtype)
        gown_ref[core, j] = value
        value = value.astype(jnp.float32)
        line = jnp.sum(value * value, axis=0, keepdims=True)
        lanes = sq_ref.shape[-1]
        fold = line[:, :lanes]
        for i in range(1, cols // lanes):
            fold = fold + line[:, i * lanes : (i + 1) * lanes]
        sq_ref[0, me, j] = fold
        return carry

    lax.fori_loop(0, members, add_last, 0)
    fourth = []
    for k, peer in enumerate(near):
        c = remote(sq_ref.at[0, me], sq_ref.at[0, me], gs.at[k], gr.at[k], (peer, z))
        c.start()
        fourth.append(c)
    c = remote(gown_ref.at[core], gown_ref.at[core], gs.at[len(near)], gr.at[len(near)], (to_core, z))
    c.start()
    for f in fourth:
        f.wait_recv()
    for d in range(1, n_shard):
        f = remote(
            sq_ref.at[0], sq_ref.at[d], qs.at[d - 1], qr.at[d - 1],
            (me, lax.rem(z + d, n_shard)),
        )
        f.start()
        fourth.append(f)
    for f in fourth[len(near):]:
        f.wait_recv()
    c.wait_recv()
    for f in fourth + [c]:
        f.wait_send()
    for c in first + second + third:
        c.wait_send()


def spread_kernel(
    n_shard, mat_ref, place_ref, factor_ref, momentum_ref, gown_ref, full_ref, gall_ref,
    held, zs, zr, cs, cr, gs, gr,
):
    me, core, x, y, to_core, to_x, to_y, to_xy = place()
    z = lax.axis_index("shard")
    rows = full_ref.shape[0] // 2
    cols = full_ref.shape[1] // n_shard

    def at(side, shard):
        return (
            pl.ds(pl.multiple_of(side * rows, rows), rows),
            pl.ds(pl.multiple_of(shard * cols, cols), cols),
        )

    def nesterov(p, side):
        matrix = mat_ref[p]
        half = pl.ds(pl.multiple_of(side * rows, rows), rows)
        step = factor_ref[matrix] * gown_ref[side, place_ref[p]].astype(jnp.float32)
        new = momentum_rate * momentum_ref[matrix, half] + step
        return (step + momentum_rate * new).astype(full_ref.dtype)

    order = [d for d in (2, 1, 3) if d < n_shard] + list(range(4, n_shard))
    for d in order:
        held[d - 1] = nesterov(lax.rem(z + d, n_shard), core)
    gall_ref[me] = gown_ref[core]
    greet(
        [(p, z) for p in (to_core, to_x, to_y)]
        + [(me, lax.rem(z + d, n_shard)) for d in range(1, n_shard)]
    )
    copies = []
    for d in order:
        peer = (me, lax.rem(z + d, n_shard))
        c = remote(held.at[d - 1], full_ref.at[at(core, z)], zs.at[d - 1], zr.at[d - 1], peer)
        c.start()
        copies.append(c)
    at_g = block_at(gall_ref, 2)
    gathers = plane_gather_start(z, at_g, gs, gr)
    for side in range(2):
        full_ref[at(side, z)] = nesterov(z, side)
    onward = []
    for c, d in zip(copies, order):
        c.wait_recv()
        source = full_ref.at[at(core, lax.rem(z + n_shard - d, n_shard))]
        f = remote(source, source, cs.at[d - 1], cr.at[d - 1], (to_core, z))
        f.start()
        onward.append(f)
        if len(onward) == 1:
            plane_gather_turn(z, at_g, gs, gr, gathers)
    for f in onward:
        f.wait_recv()
    plane_gather_finish(z, at_g, gs, gr, gathers)
    for c in copies + onward:
        c.wait_send()


def newton_kernel(u_ref, o_ref):
    def total(i, carry):
        value = u_ref[pl.ds(pl.multiple_of(i * 32, 32), 32), :].astype(jnp.float32)
        return carry + jnp.sum(value * value, axis=0, keepdims=True)

    kv, width = u_ref.shape
    sums = lax.fori_loop(0, kv // 32, total, jnp.zeros((1, width), jnp.float32))
    inverse = 1.0 / (jnp.sqrt(jnp.sum(sums, axis=1, keepdims=True)) + epsilon)
    matrix = (u_ref[...].astype(jnp.float32) * inverse).astype(jnp.bfloat16)
    for iteration in range(ITERS):
        gram = lax.dot_general(
            matrix, matrix, (((1,), (1,)), ((), ())), preferred_element_type=jnp.float32
        ).astype(jnp.bfloat16)
        square = jnp.dot(gram, gram, preferred_element_type=jnp.float32)
        mixing = (coef_b * gram.astype(jnp.float32) + coef_c * square).astype(jnp.bfloat16)
        product = jnp.dot(mixing, matrix, preferred_element_type=jnp.float32)
        matrix = (coef_a * matrix.astype(jnp.float32) + product).astype(jnp.bfloat16)
    o_ref[...] = matrix


def share_kernel(
    n_shard, owner_ref, o_ref, oall_ref, whole_ref, back, bs, br, us, ur, ws, wr
):
    me, core, x, y, to_core, to_x, to_y, to_xy = place()
    z = lax.axis_index("shard")
    rows = o_ref.shape[0] // 2
    cols = o_ref.shape[1] // n_shard
    half = pl.ds(pl.multiple_of(core * rows, rows), rows)

    def piece(shard):
        return half, pl.ds(pl.multiple_of(shard * cols, cols), cols)

    peers = [(p, z) for p in (to_core, to_x, to_y)]
    peers += [(me, lax.rem(z + d, n_shard)) for d in range(1, n_shard)]
    greet(peers)
    order = [d for d in (2, 1, 3) if d < n_shard] + list(range(4, n_shard))
    returns = []
    for d in order:
        to = lax.rem(z + d, n_shard)
        c = remote(o_ref.at[piece(to)], back.at[z], bs.at[d - 1], br.at[d - 1], (me, to))
        c.start()
        returns.append(c)
    whole_ref[me] = o_ref[half]
    at_w = block_at(whole_ref, 1)
    at_u = block_at(oall_ref, 2)
    cw = plane_gather_start(z, at_w, ws, wr)
    back[z] = o_ref[piece(z)]
    for c in returns:
        c.wait_recv()
    for j in range(oall_ref.shape[1]):
        oall_ref[me, j] = back[owner_ref[j]]
    cu = plane_gather_start(z, at_u, us, ur)
    plane_gather_turn(z, at_w, ws, wr, cw)
    plane_gather_turn(z, at_u, us, ur, cu)
    plane_gather_finish(z, at_w, ws, wr, cw)
    plane_gather_finish(z, at_u, us, ur, cu)
    for c in returns:
        c.wait_send()


def finish_kernel(
    scale, block_ref, member_ref, factor_ref, slot_ref, keep_ref,
    gall_ref, oall_ref, whole_ref, momentum_ref, mout_ref, update_ref, owned_ref,
    mbuf, ubuf, wbuf, load, msem, usem, wsem,
):
    mats = mbuf.shape[0]
    slots = wbuf.shape[0]
    rows = gall_ref.shape[2]

    def fetch(m):
        return pltpu.make_async_copy(momentum_ref.at[m], mbuf.at[m], load.at[m])

    def put(buf, out, sem, m):
        return pltpu.make_async_copy(buf.at[m], out.at[m], sem.at[m])

    def each(count, body):
        def step(m, carry):
            body(m)
            return carry

        lax.fori_loop(0, count, step, 0)

    each(mats, lambda m: fetch(m).start())

    def owned_one(s):
        for c in range(2):
            value = scale * whole_ref[slot_ref[s] + c].astype(jnp.float32)
            wbuf[s, pl.ds(c * rows, rows)] = (value * keep_ref[s].astype(jnp.float32)).astype(wbuf.dtype)
        put(wbuf, owned_ref, wsem, s).start()

    def update_one(m):
        for c in range(2):
            value = oall_ref[block_ref[m] + c, member_ref[m]].astype(jnp.float32)
            ubuf[m, pl.ds(c * rows, rows)] = scale * value
        put(ubuf, update_ref, usem, m).start()

    def momentum_one(m):
        fetch(m).wait()
        for c in range(2):
            cut = pl.ds(c * rows, rows)
            step = factor_ref[m] * gall_ref[block_ref[m] + c, member_ref[m]].astype(jnp.float32)
            mbuf[m, cut] = momentum_rate * mbuf[m, cut] + step
        put(mbuf, mout_ref, msem, m).start()

    each(slots, owned_one)
    each(mats, update_one)
    each(mats, momentum_one)
    each(slots, lambda s: put(wbuf, owned_ref, wsem, s).wait())
    each(mats, lambda m: put(ubuf, update_ref, usem, m).wait())
    each(mats, lambda m: put(mbuf, mout_ref, msem, m).wait())


def per_device_planes(activations, cotangents, momentum, owners, bucket_starts):
    n_shard = lax.axis_size("shard")
    n_rep = lax.axis_size("rep")
    layers, tok_rows, width = activations.shape
    token_total = tok_rows * n_shard * n_rep
    cols = width // n_shard
    rows = KV // 2
    lanes = math.gcd(cols, 128)
    groups = n_rep // 2
    members = MATS // groups
    slots = -(-MATS // n_shard) + 1
    update_scale = math.sqrt(max(KV, D))
    bf16, f32, i32 = jnp.bfloat16, jnp.float32, jnp.int32
    shapes = [MATS] * 5 + [n_shard] * 2 + [members] + [slots] * 2
    lay, half, position, block, member, mats, places, owner, slot_block, slot_keep = pl.pallas_call(
        functools.partial(plan_kernel, n_shard, groups),
        out_shape=[jax.ShapeDtypeStruct((n,), i32) for n in shapes],
        in_specs=[SMEM_SPEC],
        out_specs=[SMEM_SPEC] * len(shapes),
        scratch_shapes=[pltpu.SMEM((MATS,), i32), pltpu.SMEM((MATS,), i32)],
        name="plan",
    )(owners)
    index = jnp.arange(MATS, dtype=i32)

    params = functools.partial(
        pltpu.CompilerParams, has_side_effects=True, vmem_limit_bytes=VMEM_LIMIT
    )
    dma = pltpu.SemaphoreType.DMA
    gown, sq = pl.pallas_call(
        functools.partial(reduce_kernel, n_shard, 1.0 / math.sqrt(token_total)),
        out_shape=(
            jax.ShapeDtypeStruct((2, members, rows, cols), bf16),
            jax.ShapeDtypeStruct((n_shard, n_rep, members, 1, lanes), f32),
        ),
        in_specs=[SMEM_SPEC, SMEM_SPEC, ANY_SPEC, ANY_SPEC],
        out_specs=(VMEM_SPEC, VMEM_SPEC),
        scratch_shapes=[
            [pltpu.VMEM((layers, 2 * tok_rows, cols), bf16) for _ in range(n_shard)],
            pltpu.VMEM((layers, 2 * tok_rows, 2 * KV), bf16),
            pltpu.VMEM((n_shard, 2, 2, members, rows, cols), bf16),
            pltpu.VMEM((n_shard, 2, members, rows, cols), bf16),
            pltpu.VMEM((n_shard, members, rows, cols), bf16),
            pltpu.VMEM((n_shard, members, rows, cols), bf16),
            pltpu.VMEM((n_shard, members, rows, cols), bf16),
            pltpu.VMEM((n_shard - 1, members, rows, cols), bf16),
            dma((n_shard + 1,)), dma((n_shard + 1,)), dma((n_shard + 1,)),
            dma((n_shard,)), dma((n_shard,)), dma((n_shard,)), dma((n_shard,)),
            dma((n_shard,)), dma((n_shard,)),
            dma((8,)), dma((8,)), dma((n_shard - 1,)), dma((n_shard - 1,)),
        ],
        compiler_params=params(collective_id=0),
        name="reduce",
    )(lay, half, activations, cotangents)

    by_position = jnp.sum(
        sq.reshape(n_shard, groups, 2, members, lanes), axis=(0, 2, 4)
    ).reshape(MATS)
    square_sums = jnp.sum(
        jnp.where(position[:, None] == index[None, :], by_position[None, :], 0.0), axis=1
    )
    factors = clip_factors(square_sums, bucket_starts)

    full, gall = pl.pallas_call(
        functools.partial(spread_kernel, n_shard),
        out_shape=(
            jax.ShapeDtypeStruct((KV, width), bf16),
            jax.ShapeDtypeStruct((n_rep, members, rows, cols), bf16),
        ),
        in_specs=[SMEM_SPEC, SMEM_SPEC, SMEM_SPEC, VMEM_SPEC, VMEM_SPEC],
        out_specs=(VMEM_SPEC, VMEM_SPEC),
        scratch_shapes=[pltpu.VMEM((n_shard - 1, rows, cols), bf16)]
        + [dma((n_shard - 1,)) for _ in range(4)]
        + [dma((10,)) for _ in range(2)],
        compiler_params=params(collective_id=1),
        name="spread",
    )(mats, places, factors, momentum, gown)

    result = pl.pallas_call(
        newton_kernel,
        out_shape=jax.ShapeDtypeStruct((KV, width), bf16),
        in_specs=[VMEM_SPEC],
        out_specs=VMEM_SPEC,
        name="newton",
    )(full)

    oall, whole = pl.pallas_call(
        functools.partial(share_kernel, n_shard),
        out_shape=(
            jax.ShapeDtypeStruct((n_rep, members, rows, cols), bf16),
            jax.ShapeDtypeStruct((n_rep, rows, width), bf16),
        ),
        in_specs=[SMEM_SPEC, VMEM_SPEC],
        out_specs=(VMEM_SPEC, VMEM_SPEC),
        scratch_shapes=[pltpu.VMEM((n_shard, rows, cols), bf16)]
        + [dma((n_shard - 1,)) for _ in range(2)]
        + [dma((10,)) for _ in range(4)],
        compiler_params=params(collective_id=2),
        name="share",
    )(owner, result)

    momentum_out, update, owned = pl.pallas_call(
        functools.partial(finish_kernel, update_scale),
        out_shape=(
            jax.ShapeDtypeStruct(momentum.shape, f32),
            jax.ShapeDtypeStruct(momentum.shape, f32),
            jax.ShapeDtypeStruct((slots, KV, width), bf16),
        ),
        in_specs=[SMEM_SPEC] * 5 + [VMEM_SPEC] * 3 + [ANY_SPEC],
        out_specs=(ANY_SPEC,) * 3,
        scratch_shapes=[
            pltpu.VMEM(momentum.shape, f32),
            pltpu.VMEM(momentum.shape, f32),
            pltpu.VMEM((slots, KV, width), bf16),
            dma((MATS,)), dma((MATS,)), dma((MATS,)), dma((slots,)),
        ],
        compiler_params=pltpu.CompilerParams(vmem_limit_bytes=VMEM_LIMIT),
        name="finish",
    )(
        block, member, factors, slot_block, slot_keep,
        gall, oall, whole, momentum,
    )
    return (momentum_out, update, owned)


def solution(mesh):
    groups = mesh.shape["rep"] // 2
    slots = -(-MATS // mesh.shape["shard"]) + 1
    fits = mesh.shape["rep"] == 8 and MATS % groups == 0 and slots <= groups
    placed = (
        P(None, ("rep", "shard"), None),
        P(None, ("rep", "shard"), None),
        P(None, None, "shard"),
        P(),
        P(),
    )
    return jax.shard_map(
        per_device_planes if fits else per_device_general,
        mesh=mesh,
        in_specs=placed,
        out_specs=(P(None, None, "shard"), P(None, None, "shard"), P("shard", None, None)),
        check_vma=False,
    )
```
